32 devices in a mesh: seq: 8 (over z, y), batch: 4 (over x, core).
Axes of the slice: x: 2, y: 2, z: 4, core: 2. Of those that a mesh axis runs over, the one named last changes fastest.
Arguments:
- queries: bfloat16 [4, 4096, 16, 128], P('batch', 'seq'), may hold values from -5 to 5
- keys: bfloat16 [4, 4096, 16, 128], P('batch', 'seq'), may hold values from -5 to 5
- values: bfloat16 [4, 4096, 16, 128], P('batch', 'seq'), may hold values from -5 to 5
- keep_count: int32 [4, 16, 32], P('batch'), may hold values from 0 to 128
- query_map: bfloat16 [16, 128, 8], replicated, may hold values from -0.5 to 0.5
- key_map: bfloat16 [16, 128, 8], replicated, may hold values from -0.5 to 0.5
- cotangent: bfloat16 [4, 4096, 16, 128], P('batch', 'seq'), may hold values from -5 to 5
Outputs:
- attended: bfloat16 [4, 4096, 16, 128], P('batch', 'seq')
- grad_query_map: float32 [16, 128, 8], replicated
- grad_key_map: float32 [16, 128, 8], replicated
The draws below stay inside these ranges and needn't reach their ends.
All inputs are finite; a program needn't handle non-finite values.
Results may differ from the reference program's by a relative error of at most 0.0035.
Values may be sent and summed in bfloat16 or wider, within the bound.
A program may use at most 128 MiB of HBM per device.

```python
import math
import jax
import jax.numpy as jnp
from jax import lax

HEADS = 16
DH = 128
RANK = 8
TILE = 128
WINDOW = 256
LEN = 4096
SEQS = 4
TILES = 32


def draw_queries(key, part):
    base = jax.random.truncated_normal(jax.random.fold_in(key, 1), -5.0, 5.0, (SEQS, LEN, HEADS, DH), jnp.float32)
    return base.astype(jnp.bfloat16)


def draw_keys(key, part):
    base = jax.random.truncated_normal(jax.random.fold_in(key, 2), -5.0, 5.0, (SEQS, LEN, HEADS, DH), jnp.float32)
    return base.astype(jnp.bfloat16)


def touch_ends(entries, key, least, top_value):
    longest = entries.shape.index(max(entries.shape))
    spots = []
    for shift in (0, 1):
        where = [jax.random.randint(jax.random.fold_in(key, axis), (), 0, length) for axis, length in enumerate(entries.shape)]
        where[longest] = (where[longest] + shift) % entries.shape[longest]
        spots.append(tuple(where))
    return entries.at[spots[0]].set(least).at[spots[1]].set(top_value)


def shard_levels(stream_key, dims, split, low, largest):
    factor_of, own = 1.0, jax.random.fold_in(stream_key, 6)
    for axis_at, parts in split:
        heights = jnp.exp(jax.random.uniform(jax.random.fold_in(own, axis_at), (parts,), jnp.float32, low / len(split), largest / len(split)))
        factor_of = factor_of * jnp.repeat(heights, dims[axis_at] // parts).reshape([-1 if axis == axis_at else 1 for axis in range(len(dims))])
    return factor_of


def centred(key, dims, scale, bound, split=(), kind=jnp.bfloat16):
    values = scale * jax.random.normal(key, dims, jnp.float32)
    if split:
        values = values * shard_levels(key, dims, split, -0.22, 0.18)
    return jnp.clip(values, -bound, bound).astype(kind)


def setup_inputs(seed: int = 0) -> dict:
    key_of = jax.random.split(jax.random.key(seed), 8)
    queries = draw_queries(jax.random.fold_in(key_of[7], 71), 0)
    keys = draw_keys(jax.random.fold_in(key_of[7], 71), 0)
    values = centred(key_of[2], (SEQS, LEN, HEADS, DH), 1.0, 5.0, ((0, 4), (1, 8)))
    keep_count = touch_ends(jax.random.randint(key_of[3], (SEQS, HEADS, TILES), 0, TILE + 1), jax.random.fold_in(key_of[3], 1), 0, TILE).astype(jnp.int32)
    query_map = centred(key_of[4], (HEADS, DH, RANK), DH ** -0.5, 0.5)
    key_map = centred(key_of[5], (HEADS, DH, RANK), DH ** -0.5, 0.5)
    cotangent = centred(key_of[6], (SEQS, LEN, HEADS, DH), 1.0, 5.0, ((0, 4), (1, 8)))
    return {"queries": queries, "keys": keys, "values": values, "keep_count": keep_count, "query_map": query_map, "key_map": key_map, "cotangent": cotangent}


HIGHEST = lax.Precision.HIGHEST
feature_shift = 1.5

def features(inputs, weights):
    pre_act = jnp.einsum('thd,hdr->thr', inputs.astype(jnp.float32), weights, precision=HIGHEST) - feature_shift
    return jax.nn.softplus(pre_act)

def shifted(array, offset):
    filler = jnp.zeros((offset,) + array.shape[1:], array.dtype)
    return jnp.concatenate([filler, array[:array.shape[0] - offset]], 0)

def exclusive(array):
    summed = jnp.cumsum(array, 0)
    return jnp.concatenate([jnp.zeros_like(array[:1]), summed[:-1]], 0)

def sparse_part(q_rows, k_rows, v_rows, kept):
    length, heads, width = q_rows.shape
    span = WINDOW // TILE
    scale = 1.0 / math.sqrt(width)
    filler = jnp.zeros((WINDOW, heads, width), k_rows.dtype)
    k_padded = jnp.concatenate([filler, k_rows], 0)
    v_padded = jnp.concatenate([filler, v_rows], 0)
    kept_padded = jnp.concatenate([jnp.zeros((WINDOW, heads), bool), kept], 0)

    def one_block(block):
        start = (block * WINDOW).astype(jnp.int32)
        q_block = lax.dynamic_slice_in_dim(q_rows, start, WINDOW, 0)
        k_block = lax.dynamic_slice_in_dim(k_padded, start, 2 * WINDOW, 0)
        v_block = lax.dynamic_slice_in_dim(v_padded, start, 2 * WINDOW, 0)
        kept_block = lax.dynamic_slice_in_dim(kept_padded, start, 2 * WINDOW, 0)
        q_pos = start + jnp.arange(WINDOW, dtype=jnp.int32)
        k_pos = start - WINDOW + jnp.arange(2 * WINDOW, dtype=jnp.int32)
        scores = jnp.einsum('thd,phd->htp', q_block.astype(jnp.float32), k_block.astype(jnp.float32)) * scale
        tile_gap = q_pos[:, None] // TILE - k_pos[None, :] // TILE
        causal = (k_pos[None, :] <= q_pos[:, None]) & (k_pos[None, :] >= 0) & (tile_gap < span)
        live_pairs = causal[None] & ((tile_gap == 0)[None] | kept_block.T[:, None, :])
        row_max = lax.optimization_barrier(jnp.max(jnp.where(live_pairs, scores, -jnp.inf), -1))
        weights = jnp.where(live_pairs, jnp.exp(scores - row_max[..., None]), 0.0)
        denom = lax.optimization_barrier(jnp.sum(weights, -1))
        numer = jnp.einsum('htp,phd->thd', weights.astype(jnp.bfloat16).astype(jnp.float32), v_block.astype(jnp.float32))
        return (numer, denom.T, row_max.T)
    numer, denom, row_max = lax.map(one_block, jnp.arange(length // WINDOW, dtype=jnp.int32))
    return (numer.reshape(length, heads, width), denom.reshape(length, heads), row_max.reshape(length, heads))

def reference(queries, keys, values, keep_count, query_map, key_map, cotangent):
    query_weights = query_map.astype(jnp.float32)
    key_weights = key_map.astype(jnp.float32)
    span = WINDOW // TILE

    def one_sequence(inputs):
        q_rows, k_rows, v_rows, counts, cot_rows = inputs
        length, heads, width = q_rows.shape
        tiles = length // TILE
        within = jnp.arange(length, dtype=jnp.int32) % TILE
        kept = within[:, None] < jnp.repeat(counts, TILE, axis=1).T
        numer, denom, row_max = sparse_part(q_rows, k_rows, v_rows, kept)
        decay = jnp.exp(-row_max)
        v_tiles = v_rows.astype(jnp.float32).reshape(tiles, TILE, heads, width)
        evicted = (1 - kept.astype(jnp.float32)).reshape(tiles, TILE, heads, 1)

        def linear(q_weights, k_weights):
            feat_q = features(q_rows, q_weights).reshape(tiles, TILE, heads, RANK)
            feat_k = features(k_rows, k_weights).reshape(tiles, TILE, heads, RANK)
            all_state = jnp.einsum('nthr,nthd->nhrd', feat_k, v_tiles, precision=HIGHEST)
            all_norm = lax.optimization_barrier(jnp.sum(feat_k, 1))
            ev_feat = feat_k * evicted
            ev_state = jnp.einsum('nthr,nthd->nhrd', ev_feat, v_tiles, precision=HIGHEST)
            ev_norm = lax.optimization_barrier(jnp.sum(ev_feat, 1))
            state = shifted(exclusive(all_state), span - 1)
            norm = shifted(exclusive(all_norm), span - 1)
            for offset in range(1, span):
                state = state + shifted(ev_state, offset)
                norm = norm + shifted(ev_norm, offset)
            kernel_num = jnp.einsum('nthr,nhrd->nthd', feat_q, state, precision=HIGHEST).reshape(length, heads, width)
            kernel_den = jnp.einsum('nthr,nhr->nth', feat_q, norm, precision=HIGHEST).reshape(length, heads)
            return (numer + decay[..., None] * kernel_num) / (denom + decay * kernel_den)[..., None]
        out, pull_back = jax.vjp(linear, query_weights, key_weights)
        grad_q, grad_k = pull_back(cot_rows.astype(jnp.float32))
        return (out.astype(jnp.bfloat16), grad_q, grad_k)
    attended, grad_q, grad_k = lax.map(one_sequence, (queries, keys, values, keep_count, cotangent))
    return (attended, lax.optimization_barrier(jnp.sum(grad_q, 0)), lax.optimization_barrier(jnp.sum(grad_k, 0)))
```

```python
import functools
import math

import jax
import jax.numpy as jnp
from jax import lax
from jax.experimental import pallas as pl
from jax.experimental.pallas import tpu as pltpu
from jax.sharding import PartitionSpec as P

TILE = 128
SHIFT = 1.5
LOG2E = 1.0 / math.log(2.0)
MASKED = -1e30
F32 = jnp.float32
BF16 = jnp.bfloat16
GROUPS = 2
UNROLL = 4
VMEM_LIMIT = 56 * 1024 * 1024


def dot_nt(a, b):
    return lax.dot_general(a, b, (((1,), (1,)), ((), ())), preferred_element_type=F32)


def dot_nn(a, b):
    return lax.dot_general(a, b, (((1,), (0,)), ((), ())), preferred_element_type=F32)


def dot_tn(a, b):
    return lax.dot_general(a, b, (((0,), (0,)), ((), ())), preferred_element_type=F32)


def by_head(x):
    return jnp.swapaxes(x, 0, 1)


def softplus(x):
    return jnp.maximum(x, 0.0) + jnp.log1p(jnp.exp(-jnp.abs(x)))


def sigmoid(x):
    return 1.0 / (1.0 + jnp.exp(-x))


def halves(x):
    top = x.astype(BF16)
    return top, (x - top.astype(F32)).astype(BF16)


def split_dot(dot, x, y):
    rows = x.shape[0]
    both = dot(jnp.concatenate(halves(x), 0), y)
    return both[:rows] + both[rows:]


def flat_id(axes):
    index, count = 0, 1
    for axis in axes:
        index = index * lax.axis_size(axis) + lax.axis_index(axis)
        count *= lax.axis_size(axis)
    return index, count


def place(flat, axes):
    where = {}
    for axis in reversed(axes):
        size = lax.axis_size(axis)
        where[axis] = lax.rem(flat, size)
        flat = flat // size
    return where


def greet(count, me, axes):
    barrier = pltpu.get_barrier_semaphore()

    def hello(i, carry):
        pl.semaphore_signal(
            barrier, inc=1, device_id=place(lax.rem(me + i, count), axes), device_id_type=pl.DeviceIdType.MESH
        )
        return carry

    lax.fori_loop(1, count, hello, 0)
    return barrier


def at(tile, count=1):
    return pl.ds(tile * TILE, count * TILE)


def owners_of(count, chunks):
    owners = min(count, chunks)
    return owners, count // owners, chunks // owners


def layer_kernel(
    seq, axes, counts_ref, q_hbm, k_hbm, v_hbm, c_hbm, wq_ref, wk_ref, out_hbm, gq_ref, gk_ref,
    qin, kin, vin, cin, kx, vx, vt, qx, ct, oh, halo, num, rows, preq, sigk, sall, nall, skept, nkept,
    sin, nin, dsb, dnb, gaf, naf, mine, slots, grads, gslots, done,
    in_sem, halo_out, halo_in, msg_out, msg_in, red_out, red_in, back_out, back_in, out_sem,
):
    tokens, heads, width = q_hbm.shape
    rank = wq_ref.shape[1]
    tiles = tokens // TILE
    per_group = heads // GROUPS
    factor = LOG2E / math.sqrt(width)
    me = lax.axis_index(seq)
    peers = lax.axis_size(seq)
    flat, count = flat_id(axes)
    sq = (seq,)
    barrier = greet(count, flat, axes)
    base = me * tiles
    lane = lax.broadcasted_iota(jnp.int32, (1, TILE), 1)
    sub = lax.broadcasted_iota(jnp.int32, (TILE, TILE), 0)
    causal = sub <= lax.broadcasted_iota(jnp.int32, (TILE, TILE), 1)

    def load(i, hbm, vmem, n):
        return pltpu.make_async_copy(hbm.at[at(n)], vmem.at[at(n)], in_sem.at[i, n])

    loads = [(k_hbm, kin), (v_hbm, vin), (q_hbm, qin), (c_hbm, cin)]
    for i, (hbm, vmem) in enumerate(loads):
        for n in range(tiles):
            load(i, hbm, vmem, n).start()

    def loaded(i, n):
        load(i, *loads[i], n).wait()

    @pl.when(me == 0)
    def _():
        halo[...] = jnp.zeros_like(halo)

    pl.semaphore_wait(barrier, count - 1)

    def halo_copy(g, i):
        hbm = (k_hbm, v_hbm)[i]
        return pltpu.make_async_remote_copy(
            src_ref=hbm.at[pl.ds(tokens - TILE, TILE), pl.ds(g * per_group, per_group)],
            dst_ref=halo.at[g, i],
            send_sem=halo_out.at[g, i],
            recv_sem=halo_in.at[g, i],
            device_id=place(lax.rem(me + 1, peers), sq),
            device_id_type=pl.DeviceIdType.MESH,
        )

    def halo_start(g):
        @pl.when(me < peers - 1)
        def _():
            halo_copy(g, 0).start()
            halo_copy(g, 1).start()

    def count_before(h, e):
        if e:
            return counts_ref[h, base + e - 1]
        return jnp.where(me > 0, counts_ref[h, jnp.maximum(base - 1, 0)], 0)

    def message(later, g, sender, target):
        return pltpu.make_async_remote_copy(
            src_ref=mine.at[later, g],
            dst_ref=slots.at[later, g, sender],
            send_sem=msg_out.at[later, g, target],
            recv_sem=msg_in.at[later, g, sender],
            device_id=place(target, sq),
            device_id_type=pl.DeviceIdType.MESH,
        )

    def message_start(later, g, state, norm):
        packed = jnp.zeros((rank, width), F32)
        for i in range(per_group):
            mine[later, g, i] = state(g * per_group + i).astype(BF16)
            packed = jnp.where(lane == i, norm(g * per_group + i), packed)
        mine[later, g, per_group], mine[later, g, per_group + 1] = halves(packed)

        def send(p, carry):
            message(later, g, me, p).start()
            return carry

        lax.fori_loop(0 if later else me + 1, me if later else peers, send, 0)

    def message_sent(later, g):
        def sent(p, carry):
            message(later, g, me, p).wait_send()
            return carry

        lax.fori_loop(0 if later else me + 1, me if later else peers, sent, 0)

    def message_sum(later, g, state_ref, norm_ref):
        def received(p, total):
            message(later, g, p, lax.rem(me + 1, peers)).wait_recv()
            return total + slots[later, g, p].astype(F32)

        total = lax.fori_loop(
            me + 1 if later else 0, peers if later else me, received, jnp.zeros((per_group + 2, rank, width), F32)
        )
        norms = total[per_group] + total[per_group + 1]
        for i in range(per_group):
            state_ref[g * per_group + i] = total[i]
            norm = jnp.sum(jnp.where(lane == i, norms, 0.0), 1, keepdims=True)
            norm_ref[g * per_group + i] = jnp.broadcast_to(norm, (rank, width))

    def spread(x):
        return jnp.broadcast_to(jnp.sum(x, 1, keepdims=True), (rank, width))

    def over_heads(first, last, step, act):
        def block(i, carry):
            act([first + i * step + u for u in range(step)])
            return carry

        lax.fori_loop(0, (last - first) // step, block, 0)

    halo_start(0)

    for n in range(tiles):
        loaded(0, n)
        kx[:, at(n + 1)] = by_head(kin[at(n)])
    for n in range(tiles):
        loaded(1, n)
        vx[:, at(n + 1)] = by_head(vin[at(n)])

    def key_states(hs, tile_list):
        first, size = tile_list[0], len(tile_list)
        pre = [dot_nt(wk_ref[h], kx[h, at(first, size)]) - SHIFT for h in hs]
        feat = [softplus(p) for p in pre]
        for h, p in zip(hs, pre):
            sigk[h, :, at(first, size)] = sigmoid(p)
        for e in tile_list:
            cut = slice((e - first) * TILE, (e - first + 1) * TILE)
            own = [f[:, cut] for f in feat]
            if e < tiles:
                kept = [own[i] * (lane < count_before(h, e)).astype(F32) for i, h in enumerate(hs)]
                both = [split_dot(dot_nn, jnp.concatenate([o, k], 0), vx[h, at(e)]) for o, k, h in zip(own, kept, hs)]
                for i, h in enumerate(hs):
                    skept[e, h] = both[i][rank:]
                    nkept[e, h] = spread(kept[i])
            else:
                both = [split_dot(dot_nn, o, vx[h, at(e)]) for o, h in zip(own, hs)]
            if e:
                for i, h in enumerate(hs):
                    sall[e, h] = both[i][:rank]
                    nall[e, h] = spread(own[i])

    ext = list(range(1, tiles + 1))
    for g in range(GROUPS):
        over_heads(g * per_group, (g + 1) * per_group, UNROLL, lambda hs: key_states(hs, ext))
        message_start(
            0, g, lambda h: sum(sall[e, h] for e in ext), lambda h: sum(nall[e, h] for e in ext)
        )
    for g in range(1, GROUPS):
        halo_start(g)

    def flip_values(hs, tile_list):
        for h in hs:
            for e in tile_list:
                vt[h, :, at(e)] = vx[h, at(e)].T

    over_heads(0, heads, UNROLL, lambda hs: flip_values(hs, ext))
    for n in range(tiles):
        loaded(2, n)
        qx[:, at(n)] = by_head(qin[at(n)])

    def query_features(hs):
        pre = [dot_nt(wq_ref[h], qx[h]) - SHIFT for h in hs]
        for h, p in zip(hs, pre):
            preq[h] = p

    over_heads(0, heads, UNROLL, query_features)

    def sparse(hs, j):
        each = range(len(hs))
        scores = [dot_nt(kx[h, at(j - 1, 2)], qx[h, at(j - 1)]) for h in hs]
        old = [jnp.where(sub < count_before(h, j - 1), scores[i][:TILE], MASKED) for i, h in enumerate(hs)]
        own = [jnp.where(causal, scores[i][TILE:], MASKED) for i in each]
        top = [jnp.max(jnp.maximum(old[i], own[i]), 0, keepdims=True) * factor for i in each]
        old = [jnp.exp2(old[i] * factor - top[i]) for i in each]
        own = [jnp.exp2(own[i] * factor - top[i]) for i in each]
        den = [jnp.sum(old[i] + own[i], 0, keepdims=True) for i in each]
        prob = [jnp.concatenate([old[i].astype(BF16), own[i].astype(BF16)], 0) for i in each]
        numer = [dot_nn(vt[h, :, at(j - 1, 2)], prob[i]) for i, h in enumerate(hs)]
        for i, h in enumerate(hs):
            num[h, :, at(j - 1)] = numer[i]
            rows[h, 0:1, at(j - 1)] = den[i]
            rows[h, 1:2, at(j - 1)] = top[i]

    for j in range(2, tiles + 1):
        over_heads(0, heads, UNROLL, lambda hs, j=j: sparse(hs, j))

    for n in range(tiles):
        loaded(3, n)
        oh[:, at(n)] = by_head(cin[at(n)])

    def flip_cotangent(hs):
        for h in hs:
            for n in range(tiles):
                ct[h, :, at(n)] = oh[h, at(n)].T

    over_heads(0, heads, UNROLL, flip_cotangent)
    for g in range(GROUPS):
        message_sum(0, g, sin, nin)

    def combine(hs, j):
        each = range(len(hs))
        where = at(j - 1)
        pre = [preq[h, :, where] for h in hs]
        feat = [softplus(p) for p in pre]
        state = [sum([sall[e, h] for e in range(1, j)], sin[h]) - skept[j - 1, h] for h in hs]
        norm = [sum([nall[e, h] for e in range(1, j)], nin[h]) - nkept[j - 1, h] for h in hs]
        decay = [jnp.exp2(-rows[h, 1:2, where]) for h in hs]
        kernel = []
        for i in each:
            fq_top, fq_low = halves(feat[i])
            st_top, st_low = halves(state[i])
            kernel.append(
                dot_tn(jnp.concatenate([st_top, st_top, st_low], 0), jnp.concatenate([fq_top, fq_low, fq_top], 0))
            )
        den = [jnp.sum(norm[i] * feat[i], 0, keepdims=True) for i in each]
        inv = [1.0 / (rows[h, 0:1, where] + decay[i] * den[i]) for i, h in enumerate(hs)]
        out = [(num[h, :, where] + decay[i] * kernel[i]) * inv[i] for i, h in enumerate(hs)]
        grad = [ct[h, :, where].astype(F32) * (decay[i] * inv[i]) for i, h in enumerate(hs)]
        dot = [jnp.sum(grad[i] * out[i], 0, keepdims=True) for i in each]
        grad = [x.astype(BF16) for x in grad]
        for i, h in enumerate(hs):
            oh[h, where] = out[i].astype(BF16).T
        d_fq = [split_dot(dot_nn, state[i], grad[i]) - norm[i] * dot[i] for i in each]
        ds = [split_dot(dot_nt, feat[i], grad[i]) for i in each]
        gq = [split_dot(dot_nn, d_fq[i] * sigmoid(pre[i]), qx[h, where]) for i, h in enumerate(hs)]
        for i, h in enumerate(hs):
            dsb[j, h] = ds[i]
            dnb[j, h] = -spread(feat[i] * dot[i])
            slot = (h // per_group, lax.rem(h, per_group))
            if j == tiles:
                grads[slot] = gq[i]
            else:
                grads[slot] += gq[i]

    def put_out(n):
        return pltpu.make_async_copy(qin.at[at(n)], out_hbm.at[at(n)], out_sem.at[n])

    def write_out(n):
        qin[at(n)] = by_head(oh[:, at(n)])
        put_out(n).start()

    for j in range(tiles, 1, -1):
        over_heads(0, heads, UNROLL, lambda hs, j=j: combine(hs, j))

    def local_keys(hs):
        parts = [[] for _ in hs]
        for e in range(tiles):
            later = None
            if 0 < e < tiles - 1:
                later = [sum(dsb[j, h] for j in range(e + 2, tiles + 1)) for h in hs]
            near = [dsb[e + 1, h] for h in hs]
            kept = [(lane < count_before(h, e)).astype(F32) for h in hs]
            for i, h in enumerate(hs):
                values = vt[h, :, at(e)]
                if e == 0:
                    part = -kept[i] * (split_dot(dot_nn, near[i], values) + dnb[1, h])
                elif later is None:
                    part = (1.0 - kept[i]) * (split_dot(dot_nn, near[i], values) + dnb[e + 1, h])
                else:
                    both = split_dot(dot_nn, jnp.concatenate([near[i], later[i]], 0), values)
                    far = both[rank:] + sum(dnb[j, h] for j in range(e + 2, tiles + 1))
                    part = (1.0 - kept[i]) * (both[:rank] + dnb[e + 1, h]) + far
                parts[i].append(part * sigk[h, :, at(e)])
        for i, h in enumerate(hs):
            slot = (h // per_group, per_group + lax.rem(h, per_group))
            grads[slot] = split_dot(dot_nn, jnp.concatenate(parts[i], 1), kx[h, at(0, tiles)])

    def final_keys(hs):
        own = at(1, tiles)
        d_fk = [split_dot(dot_nn, gaf[h], vt[h, :, own]) + naf[h][:, :1] for h in hs]
        gk = [split_dot(dot_nn, d_fk[i] * sigk[h, :, own], kx[h, own]) for i, h in enumerate(hs)]
        for i, h in enumerate(hs):
            grads[h // per_group, per_group + lax.rem(h, per_group)] += gk[i]

    chunks = 2 * per_group
    owners, stride, per = owners_of(count, chunks)

    def owner_id(g, o):
        return o * stride + g % stride

    def is_owner(g):
        return lax.rem(flat, stride) == g % stride

    part = flat // stride

    def to_owner(g, o, sender):
        return pltpu.make_async_remote_copy(
            src_ref=grads.at[g, pl.ds(o * per, per)],
            dst_ref=gslots.at[g, sender],
            send_sem=red_out.at[g, o],
            recv_sem=red_in.at[g, sender],
            device_id=place(owner_id(g, o), axes),
            device_id_type=pl.DeviceIdType.MESH,
        )

    def to_all(g, o, target):
        return pltpu.make_async_remote_copy(
            src_ref=done.at[g, pl.ds(o * per, per)],
            dst_ref=done.at[g, pl.ds(o * per, per)],
            send_sem=back_out.at[g, target],
            recv_sem=back_in.at[g, o],
            device_id=place(target, axes),
            device_id_type=pl.DeviceIdType.MESH,
        )

    def over_owners(g, act):
        def step(i, carry):
            o = lax.rem(part + i, owners)

            @pl.when(owner_id(g, o) != flat)
            def _():
                act(o)

            return carry

        lax.fori_loop(0, owners, step, 0)

    def reduce_start(g):
        over_owners(g, lambda o: to_owner(g, o, flat).start())

    def reduce_own(g):
        @pl.when(is_owner(g))
        def _():
            def arrived(i, total):
                sender = lax.rem(flat + i, count)
                to_owner(g, part, sender).wait_recv()
                return total + gslots[g, sender]

            done[g, pl.ds(part * per, per)] = lax.fori_loop(1, count, arrived, grads[g, pl.ds(part * per, per)])

            def send(i, carry):
                to_all(g, part, lax.rem(flat + i, count)).start()
                return carry

            lax.fori_loop(1, count, send, 0)

    def reduce_end(g):
        over_owners(g, lambda o: to_all(g, o, lax.rem(flat + 1, count)).wait_recv())
        over_owners(g, lambda o: to_owner(g, o, flat).wait_send())

        @pl.when(is_owner(g))
        def _():
            def sent(i, carry):
                to_all(g, part, lax.rem(flat + i, count)).wait_send()
                return carry

            lax.fori_loop(1, count, sent, 0)

        for i in range(per_group):
            gq_ref[g * per_group + i] = done[g, i]
            gk_ref[g * per_group + i] = done[g, per_group + i]

    for n in range(1, tiles):
        write_out(n)

    for g in range(GROUPS):
        @pl.when(me > 0)
        def _(g=g):
            halo_copy(g, 0).wait_recv()
            halo_copy(g, 1).wait_recv()

        group = slice(g * per_group, (g + 1) * per_group)
        kx[group, at(0)] = by_head(halo[g, 0])
        vx[group, at(0)] = by_head(halo[g, 1])

        def first_tile(hs):
            flip_values(hs, [0])
            key_states(hs, [0])
            sparse(hs, 1)
            combine(hs, 1)

        over_heads(g * per_group, (g + 1) * per_group, UNROLL, first_tile)
        every = range(1, tiles + 1)
        message_start(
            1, g, lambda h: sum(dsb[j, h] for j in every), lambda h: sum(dnb[j, h] for j in every)
        )
        over_heads(g * per_group, (g + 1) * per_group, UNROLL, local_keys)
    write_out(0)
    for g in range(GROUPS):
        message_sum(1, g, gaf, naf)
        over_heads(g * per_group, (g + 1) * per_group, UNROLL, final_keys)
        reduce_start(g)
    for g in range(GROUPS):
        reduce_own(g)
    for g in range(GROUPS):
        reduce_end(g)
    for g in range(GROUPS):
        @pl.when(me < peers - 1)
        def _(g=g):
            halo_copy(g, 0).wait_send()
            halo_copy(g, 1).wait_send()

        message_sent(0, g)
        message_sent(1, g)
    for n in range(tiles):
        put_out(n).wait()


def body(queries, keys, values, keep_count, query_map, key_map, cotangent):
    q_rows, k_rows, v_rows, cot = queries[0], keys[0], values[0], cotangent[0]
    tokens, heads, width = q_rows.shape
    rank = query_map.shape[2]
    tiles = tokens // TILE
    wq = jnp.swapaxes(query_map, 1, 2)
    wk = jnp.swapaxes(key_map, 1, 2)
    axes = ("seq", "batch")
    peers = lax.axis_size("seq")
    count = peers * lax.axis_size("batch")
    per_group = heads // GROUPS
    chunks = 2 * per_group
    owners, _, per = owners_of(count, chunks)
    block = (per_group + 2, rank, width)
    hbm = pl.BlockSpec(memory_space=pl.ANY)
    vmem = pl.BlockSpec(memory_space=pltpu.VMEM)
    smem = pl.BlockSpec(memory_space=pltpu.SMEM)
    dma = pltpu.SemaphoreType.DMA
    small = pltpu.VMEM((heads, rank, width), F32)
    tiled = pltpu.VMEM((tiles + 1, heads, rank, width), F32)
    out, gq, gk = pl.pallas_call(
        functools.partial(layer_kernel, "seq", axes),
        name="layer",
        in_specs=[smem, hbm, hbm, hbm, hbm, vmem, vmem],
        out_specs=[hbm, vmem, vmem],
        out_shape=[
            jax.ShapeDtypeStruct((tokens, heads, width), BF16),
            jax.ShapeDtypeStruct((heads, rank, width), F32),
            jax.ShapeDtypeStruct((heads, rank, width), F32),
        ],
        scratch_shapes=[pltpu.VMEM((tokens, heads, width), BF16)] * 4
        + [pltpu.VMEM((heads, tokens + TILE, width), BF16)] * 2
        + [
            pltpu.VMEM((heads, width, tokens + TILE), BF16),
            pltpu.VMEM((heads, tokens, width), BF16),
            pltpu.VMEM((heads, width, tokens), BF16),
            pltpu.VMEM((heads, tokens, width), BF16),
            pltpu.VMEM((GROUPS, 2, TILE, per_group, width), BF16),
            pltpu.VMEM((heads, width, tokens), F32),
            pltpu.VMEM((heads, 8, tokens), F32),
            pltpu.VMEM((heads, rank, tokens), F32),
            pltpu.VMEM((heads, rank, tokens + TILE), F32),
            tiled, tiled, tiled, tiled, small, small, tiled, tiled, small, small,
            pltpu.VMEM((2, GROUPS) + block, BF16),
            pltpu.VMEM((2, GROUPS, peers) + block, BF16),
            pltpu.VMEM((GROUPS, chunks, rank, width), F32),
            pltpu.VMEM((GROUPS, count, per, rank, width), F32),
            pltpu.VMEM((GROUPS, chunks, rank, width), F32),
            dma((4, tiles)), dma((GROUPS, 2)), dma((GROUPS, 2)), dma((2, GROUPS, peers)), dma((2, GROUPS, peers)),
            dma((GROUPS, owners)), dma((GROUPS, count)), dma((GROUPS, count)), dma((GROUPS, owners)), dma((tiles,)),
        ],
        compiler_params=pltpu.CompilerParams(
            collective_id=0, has_side_effects=True, vmem_limit_bytes=VMEM_LIMIT
        ),
    )(keep_count[0], q_rows, k_rows, v_rows, cot, wq, wk)
    return out[None], jnp.swapaxes(gq, 1, 2), jnp.swapaxes(gk, 1, 2)


def solution(mesh):
    placed = (
        P("batch", "seq", None, None),
        P("batch", "seq", None, None),
        P("batch", "seq", None, None),
        P("batch", None, None),
        P(),
        P(),
        P("batch", "seq", None, None),
    )
    return jax.shard_map(
        body,
        mesh=mesh,
        in_specs=placed,
        out_specs=(P("batch", "seq", None, None), P(), P()),
        check_vma=False,
    )
```

```python
import functools
import math

import jax
import jax.numpy as jnp
from jax import lax
from jax.experimental import pallas as pl
from jax.experimental.pallas import tpu as pltpu
from jax.sharding import PartitionSpec as P

TILE = 128
SHIFT = 1.5
LOG2E = 1.0 / math.log(2.0)
MASKED = -1e30
F32 = jnp.float32
BF16 = jnp.bfloat16
GROUPS = 2
UNROLL = 4
EARLY_EVEN = 4
EARLY_ODD = 1
PIECES = 4
VMEM_LIMIT = 58 * 1024 * 1024


def dot_nt(a, b):
    return lax.dot_general(a, b, (((1,), (1,)), ((), ())), preferred_element_type=F32)


def dot_nn(a, b):
    return lax.dot_general(a, b, (((1,), (0,)), ((), ())), preferred_element_type=F32)


def dot_tn(a, b):
    return lax.dot_general(a, b, (((0,), (0,)), ((), ())), preferred_element_type=F32)


def by_head(x):
    return jnp.swapaxes(x, 0, 1)


def softplus(x):
    return jnp.maximum(x, 0.0) + jnp.log1p(jnp.exp(-jnp.abs(x)))


def sigmoid(x):
    return 1.0 / (1.0 + jnp.exp(-x))


def halves(x):
    top = x.astype(BF16)
    return top, (x - top.astype(F32)).astype(BF16)


def split_dot(dot, x, y):
    rows = x.shape[0]
    both = dot(jnp.concatenate(halves(x), 0), y)
    return both[:rows] + both[rows:]


def flat_id(axes):
    index, count = 0, 1
    for axis in axes:
        index = index * lax.axis_size(axis) + lax.axis_index(axis)
        count *= lax.axis_size(axis)
    return index, count


def place(flat, axes):
    where = {}
    for axis in reversed(axes):
        size = lax.axis_size(axis)
        where[axis] = lax.rem(flat, size)
        flat = flat // size
    return where


def greet(count, me, axes):
    barrier = pltpu.get_barrier_semaphore()

    def hello(i, carry):
        pl.semaphore_signal(
            barrier, inc=1, device_id=place(lax.rem(me + i, count), axes), device_id_type=pl.DeviceIdType.MESH
        )
        return carry

    lax.fori_loop(1, count, hello, 0)
    return barrier


def at(tile, count=1):
    return pl.ds(tile * TILE, count * TILE)


def owners_of(count, chunks):
    owners = min(count, chunks)
    return owners, chunks // owners


def layer_kernel(
    seq, axes, counts_hbm, q_hbm, k_hbm, v_hbm, c_hbm, wq_hbm, wk_hbm, out_ref, sums_ref,
    qin, kin, vin, cin, kx, vx, vt, qx, ct, oh, halo, num, rows, preq, sigk, sall, nall, skept, nkept,
    sin, nin, dsb, dnb, gaf, naf, counts_ref, wq_ref, wk_ref, prob, fkept,
    own, state_out, state_in, even_in, mine, slots, grads, gslots, done,
    in_sem, small_sem, halo_out, halo_in, pair_out, pair_in, even_out_sem, even_in_sem,
    msg_out, msg_in, red_out, red_in, back_out, back_in, out_sem,
):
    tokens, heads, width = q_hbm.shape
    rank = wq_hbm.shape[1]
    tiles = tokens // TILE
    per_group = heads // GROUPS
    factor = LOG2E / math.sqrt(width)
    me = lax.axis_index(seq)
    peers = lax.axis_size(seq)
    flat, count = flat_id(axes)
    sq = (seq,)
    barrier = greet(count, flat, axes)
    base = me * tiles
    lane = lax.broadcasted_iota(jnp.int32, (1, TILE), 1)
    sub = lax.broadcasted_iota(jnp.int32, (TILE, TILE), 0)
    causal = sub <= lax.broadcasted_iota(jnp.int32, (TILE, TILE), 1)

    pairs_in = [(k_hbm, kin), (v_hbm, vin), (q_hbm, qin), (c_hbm, cin)]
    loads = [pltpu.make_async_copy(hbm, vmem, in_sem.at[i]) for i, (hbm, vmem) in enumerate(pairs_in)]
    for copy in loads:
        copy.start()

    smalls = [
        pltpu.make_async_copy(counts_hbm, counts_ref, small_sem.at[0]),
        pltpu.make_async_copy(wk_hbm, wk_ref, small_sem.at[1]),
        pltpu.make_async_copy(wq_hbm, wq_ref, small_sem.at[2]),
    ]
    for copy in smalls:
        copy.start()

    @pl.when(me == 0)
    def _():
        halo[...] = jnp.zeros_like(halo)
        state_in[0] = jnp.zeros_like(state_in[0])

    even = lax.rem(me, 2) == 0
    half = TILE // 2
    pieces = [(g, i, r) for g in range(GROUPS) for i in range(2) for r in range(2)]

    def halo_copy(g, i, r):
        hbm = (k_hbm, v_hbm)[i]
        return pltpu.make_async_remote_copy(
            src_ref=hbm.at[pl.ds(tokens - TILE + r * half, half), pl.ds(g * per_group, per_group)],
            dst_ref=halo.at[g, i, pl.ds(r * half, half)],
            send_sem=halo_out,
            recv_sem=halo_in.at[g, i],
            device_id=place(lax.rem(me + 1, peers), sq),
            device_id_type=pl.DeviceIdType.MESH,
        )

    def whole_copy(ref, send_sem, recv_sem):
        return pltpu.make_async_remote_copy(
            src_ref=ref,
            dst_ref=ref,
            send_sem=send_sem,
            recv_sem=recv_sem,
            device_id=place(lax.rem(me + 1, peers), sq),
            device_id_type=pl.DeviceIdType.MESH,
        )

    def halo_wait(g, i):
        @pl.when(me > 0)
        def _():
            whole_copy(halo.at[g, i], halo_out, halo_in.at[g, i]).wait_recv()

    with jax.named_scope("barrier"):
        pl.semaphore_wait(barrier, count - 1)

    def halo_start(mine, some):
        @pl.when(mine & (me < peers - 1))
        def _():
            for piece in some:
                halo_copy(*piece).start()

    odd = jnp.logical_not(even)
    halo_start(even, pieces[:EARLY_EVEN])
    halo_start(odd, pieces[:EARLY_ODD])

    def count_before(h, e):
        if e:
            return counts_ref[h, base + e - 1]
        return jnp.where(me > 0, counts_ref[h, jnp.maximum(base - 1, 0)], 0)

    def pair_copy(i, target):
        return pltpu.make_async_remote_copy(
            src_ref=state_out.at[i],
            dst_ref=state_in.at[i],
            send_sem=pair_out.at[i],
            recv_sem=pair_in.at[i],
            device_id=place(target, sq),
            device_id_type=pl.DeviceIdType.MESH,
        )

    def even_copy(sender, target):
        return pltpu.make_async_remote_copy(
            src_ref=state_out.at[2],
            dst_ref=even_in.at[sender],
            send_sem=even_out_sem.at[target],
            recv_sem=even_in_sem.at[sender],
            device_id=place(2 * target, sq),
            device_id_type=pl.DeviceIdType.MESH,
        )

    def pack(i, total):
        state_out[i, :heads] = total[:heads].astype(BF16)
        state_out[i, heads], state_out[i, heads + 1] = halves(total[heads] + total[heads + 1])

    def set_states(total):
        norms = total[heads] + total[heads + 1]
        for h in range(heads):
            sin[h] = total[h]
            nin[h] = spread(jnp.where(lane == h, norms, 0.0))

    pair, pairs = me // 2, peers // 2

    def own_states():
        packed = jnp.zeros((rank, width), F32)
        for h in range(heads):
            own[h] = sum(sall[e, h] for e in ext)
            packed = jnp.where(lane == h, sum(nall[e, h] for e in ext), packed)
        own[heads] = packed
        own[heads + 1] = jnp.zeros((rank, width), F32)

        @pl.when(odd & (me < peers - 1))
        def _():
            pack(0, own[...])
            pair_copy(0, me + 1).start()

        halo_start(odd, pieces[EARLY_ODD:])

    def pair_states():
        @pl.when(even)
        def _():
            @pl.when(me > 0)
            def _():
                pair_copy(0, me + 1).wait_recv()

            pack(2, own[...] + state_in[0].astype(F32))

            def send(p, carry):
                even_copy(pair, p).start()
                return carry

            lax.fori_loop(pair + 1, pairs, send, 0)

    def even_states():
        @pl.when(even)
        def _():
            def received(p, total):
                even_copy(p, lax.rem(pair + 1, pairs)).wait_recv()
                return total + even_in[p].astype(F32)

            total = lax.fori_loop(0, pair, received, state_in[0].astype(F32))
            pack(1, own[...] + total)
            pair_copy(1, me + 1).start()

            halo_start(even, pieces[EARLY_EVEN:])
            set_states(total)

    def odd_states():
        @pl.when(odd)
        def _():
            pair_copy(1, me - 1).wait_recv()
            set_states(state_in[1].astype(F32))

    def states_sent():
        @pl.when(even)
        def _():
            def sent(p, carry):
                even_copy(pair, p).wait_send()
                return carry

            lax.fori_loop(pair + 1, pairs, sent, 0)
            pair_copy(1, me + 1).wait_send()

        @pl.when(odd & (me < peers - 1))
        def _():
            pair_copy(0, me + 1).wait_send()

    def message(g, sender, target):
        return pltpu.make_async_remote_copy(
            src_ref=mine.at[g],
            dst_ref=slots.at[g, sender],
            send_sem=msg_out.at[g, target],
            recv_sem=msg_in.at[g, sender],
            device_id=place(target, sq),
            device_id_type=pl.DeviceIdType.MESH,
        )

    def message_start(g):
        every = range(1, tiles + 1)
        packed = jnp.zeros((rank, width), F32)
        for i in range(per_group):
            h = g * per_group + i
            mine[g, i] = sum(dsb[j, h] for j in every).astype(BF16)
            packed = jnp.where(lane == i, sum(dnb[j, h] for j in every), packed)
        mine[g, per_group], mine[g, per_group + 1] = halves(packed)

        def send(p, carry):
            message(g, me, p).start()
            return carry

        lax.fori_loop(0, me, send, 0)

    def message_sent(g):
        def sent(p, carry):
            message(g, me, p).wait_send()
            return carry

        lax.fori_loop(0, me, sent, 0)

    def message_sum(g):
        def received(p, total):
            message(g, p, lax.rem(me + 1, peers)).wait_recv()
            return total + slots[g, p].astype(F32)

        total = lax.fori_loop(me + 1, peers, received, jnp.zeros((per_group + 2, rank, width), F32))
        norms = total[per_group] + total[per_group + 1]
        for i in range(per_group):
            gaf[g * per_group + i] = total[i]
            naf[g * per_group + i] = spread(jnp.where(lane == i, norms, 0.0))

    def spread(x):
        return jnp.broadcast_to(jnp.sum(x, 1, keepdims=True), (rank, width))

    def over_heads(first, last, step, act):
        def block(i, carry):
            act([first + i * step + u for u in range(step)])
            return carry

        lax.fori_loop(0, (last - first) // step, block, 0)

    ext = list(range(1, tiles + 1))
    with jax.named_scope("keys"):
        loads[0].wait()
        for n in range(tiles):
            kx[:, at(n + 1)] = by_head(kin[at(n)])
    with jax.named_scope("values"):
        loads[1].wait()
        for n in range(tiles):
            vx[:, at(n + 1)] = by_head(vin[at(n)])
    with jax.named_scope("maps"):
        for copy in smalls:
            copy.wait()

    def key_features(hs, tile_list):
        where = at(tile_list[0], len(tile_list))
        pre = [dot_nt(wk_ref[h], kx[h, where]) - SHIFT for h in hs]
        for h, p in zip(hs, pre):
            sigk[h, :, where] = sigmoid(p)
        return [softplus(p) for p in pre]

    def kept_part(hs, e, feat):
        return [f * (lane < count_before(h, e)).astype(F32) for f, h in zip(feat, hs)]

    def key_states(hs):
        feat = key_features(hs, ext)
        for e in ext:
            one = [f[:, (e - 1) * TILE : e * TILE] for f in feat]
            if e < tiles:
                kept = kept_part(hs, e, one)
                both = [split_dot(dot_nn, jnp.concatenate([o, k], 0), vx[h, at(e)]) for o, k, h in zip(one, kept, hs)]
                for i, h in enumerate(hs):
                    skept[e, h] = both[i][rank:]
                    nkept[e, h] = spread(kept[i])
            else:
                both = [split_dot(dot_nn, o, vx[h, at(e)]) for o, h in zip(one, hs)]
            for i, h in enumerate(hs):
                sall[e, h] = both[i][:rank]
                nall[e, h] = spread(one[i])

    with jax.named_scope("states"):
        over_heads(0, heads, UNROLL, key_states)
        own_states()

    def flip_values(hs, tile_list):
        for h in hs:
            for e in tile_list:
                vt[h, :, at(e)] = vx[h, at(e)].T

    with jax.named_scope("flip_v"):
        over_heads(0, heads, UNROLL, lambda hs: flip_values(hs, ext))
    with jax.named_scope("queries"):
        loads[2].wait()
        for n in range(tiles):
            qx[:, at(n)] = by_head(qin[at(n)])

    def query_features(hs):
        pre = [dot_nt(wq_ref[h], qx[h]) - SHIFT for h in hs]
        for h, p in zip(hs, pre):
            preq[h] = p

    with jax.named_scope("qfeat"):
        over_heads(0, heads, UNROLL, query_features)
    def weights(hs, j):
        each = range(len(hs))
        scores = [dot_nt(kx[h, at(j - 1, 2)], qx[h, at(j - 1)]) for h in hs]
        old = [jnp.where(sub < count_before(h, j - 1), scores[i][:TILE], MASKED) for i, h in enumerate(hs)]
        new = [jnp.where(causal, scores[i][TILE:], MASKED) for i in each]
        top = [jnp.max(jnp.maximum(old[i], new[i]), 0, keepdims=True) * factor for i in each]
        old = [jnp.exp2(old[i] * factor - top[i]) for i in each]
        new = [jnp.exp2(new[i] * factor - top[i]) for i in each]
        for i, h in enumerate(hs):
            rows[h, 0:1, at(j - 1)] = jnp.sum(old[i] + new[i], 0, keepdims=True)
            rows[h, 1:2, at(j - 1)] = top[i]
        return [jnp.concatenate([old[i].astype(BF16), new[i].astype(BF16)], 0) for i in each]

    def weighted(hs, j, weight):
        numer = [dot_nn(vt[h, :, at(j - 1, 2)], w) for h, w in zip(hs, weight)]
        for h, x in zip(hs, numer):
            num[h, :, at(j - 1)] = x

    def sparse(hs, j):
        weighted(hs, j, weights(hs, j))

    with jax.named_scope("sparse"):
        for j in range(2, tiles + 1):
            over_heads(0, heads, UNROLL, lambda hs, j=j: sparse(hs, j))
            if j == 2:
                with jax.named_scope("pair_states"):
                    pair_states()
    with jax.named_scope("even_states"):
        even_states()
    with jax.named_scope("cot"):
        loads[3].wait()
        for n in range(tiles):
            oh[:, at(n)] = by_head(cin[at(n)])

    def flip_cotangent(hs):
        for h in hs:
            for n in range(tiles):
                ct[h, :, at(n)] = oh[h, at(n)].T

    with jax.named_scope("flip_c"):
        over_heads(0, heads, UNROLL, flip_cotangent)
    with jax.named_scope("odd_states"):
        odd_states()

    def combine(hs, j):
        each = range(len(hs))
        where = at(j - 1)
        pre = [preq[h, :, where] for h in hs]
        feat = [softplus(p) for p in pre]
        state = [sum([sall[e, h] for e in range(1, j)], sin[h]) - skept[j - 1, h] for h in hs]
        norm = [sum([nall[e, h] for e in range(1, j)], nin[h]) - nkept[j - 1, h] for h in hs]
        decay = [jnp.exp2(-rows[h, 1:2, where]) for h in hs]
        kernel = []
        for i in each:
            fq_top, fq_low = halves(feat[i])
            st_top, st_low = halves(state[i])
            kernel.append(
                dot_tn(jnp.concatenate([st_top, st_top, st_low], 0), jnp.concatenate([fq_top, fq_low, fq_top], 0))
            )
        den = [jnp.sum(norm[i] * feat[i], 0, keepdims=True) for i in each]
        inv = [1.0 / (rows[h, 0:1, where] + decay[i] * den[i]) for i, h in enumerate(hs)]
        out = [(num[h, :, where] + decay[i] * kernel[i]) * inv[i] for i, h in enumerate(hs)]
        grad = [ct[h, :, where].astype(F32) * (decay[i] * inv[i]) for i, h in enumerate(hs)]
        dot = [jnp.sum(grad[i] * out[i], 0, keepdims=True) for i in each]
        grad = [x.astype(BF16) for x in grad]
        for i, h in enumerate(hs):
            oh[h, where] = out[i].astype(BF16).T
        d_fq = [split_dot(dot_nn, state[i], grad[i]) - norm[i] * dot[i] for i in each]
        ds = [split_dot(dot_nt, feat[i], grad[i]) for i in each]
        gq = [split_dot(dot_nn, d_fq[i] * sigmoid(pre[i]), qx[h, where]) for i, h in enumerate(hs)]
        for i, h in enumerate(hs):
            dsb[j, h] = ds[i]
            dnb[j, h] = -spread(feat[i] * dot[i])
            slot = (h // per_group, lax.rem(h, per_group))
            if j == tiles:
                grads[slot] = gq[i]
            else:
                grads[slot] += gq[i]

    with jax.named_scope("combine"):
        for j in range(tiles, 1, -1):
            over_heads(0, heads, UNROLL, lambda hs, j=j: combine(hs, j))

    def local_keys(hs):
        parts = [[] for _ in hs]
        for e in range(tiles):
            later = None
            if 0 < e < tiles - 1:
                later = [sum(dsb[j, h] for j in range(e + 2, tiles + 1)) for h in hs]
            near = [dsb[e + 1, h] for h in hs]
            kept = [(lane < count_before(h, e)).astype(F32) for h in hs]
            for i, h in enumerate(hs):
                values = vt[h, :, at(e)]
                if e == 0:
                    part = -kept[i] * (split_dot(dot_nn, near[i], values) + dnb[1, h])
                elif later is None:
                    part = (1.0 - kept[i]) * (split_dot(dot_nn, near[i], values) + dnb[e + 1, h])
                else:
                    both = split_dot(dot_nn, jnp.concatenate([near[i], later[i]], 0), values)
                    far = both[rank:] + sum(dnb[j, h] for j in range(e + 2, tiles + 1))
                    part = (1.0 - kept[i]) * (both[:rank] + dnb[e + 1, h]) + far
                parts[i].append(part * sigk[h, :, at(e)])
        for i, h in enumerate(hs):
            slot = (h // per_group, per_group + lax.rem(h, per_group))
            grads[slot] = split_dot(dot_nn, jnp.concatenate(parts[i], 1), kx[h, at(0, tiles)])

    def final_keys(hs):
        own = at(1, tiles)
        d_fk = [split_dot(dot_nn, gaf[h], vt[h, :, own]) + naf[h][:, :1] for h in hs]
        gk = [split_dot(dot_nn, d_fk[i] * sigk[h, :, own], kx[h, own]) for i, h in enumerate(hs)]
        for i, h in enumerate(hs):
            grads[h // per_group, per_group + lax.rem(h, per_group)] += gk[i]

    chunks = 2 * per_group
    owners, per = owners_of(count, chunks)

    def owner_id(g, o):
        return middle + o

    def is_owner(g):
        return (flat >= middle) & (flat < middle + owners)

    middle = (count - owners) // 2
    part = lax.rem(flat - middle + count, owners)

    def to_owner(g, o, sender):
        return pltpu.make_async_remote_copy(
            src_ref=grads.at[g, pl.ds(o * per, per)],
            dst_ref=gslots.at[g, lax.rem(sender - owner_id(g, o) + count - 1, count)],
            send_sem=red_out.at[g],
            recv_sem=red_in.at[g],
            device_id=place(owner_id(g, o), axes),
            device_id_type=pl.DeviceIdType.MESH,
        )

    def to_all(g, o, target):
        return pltpu.make_async_remote_copy(
            src_ref=done.at[g, pl.ds(o * per, per)],
            dst_ref=done.at[g, pl.ds(o * per, per)],
            send_sem=back_out.at[g],
            recv_sem=back_in.at[g],
            device_id=place(target, axes),
            device_id_type=pl.DeviceIdType.MESH,
        )

    def over_owners(g, act):
        def step(i, carry):
            o = lax.rem(part + i, owners)

            @pl.when(owner_id(g, o) != flat)
            def _():
                act(o)

            return carry

        lax.fori_loop(0, owners, step, 0)

    def reduce_start(g):
        over_owners(g, lambda o: to_owner(g, o, flat).start())

    def reduce_own(g):
        @pl.when(is_owner(g))
        def _():
            whole_copy(gslots.at[g], red_out.at[g], red_in.at[g]).wait_recv()
            mine_now = pl.ds(part * per, per)
            done[g, mine_now] = lax.fori_loop(0, count - 1, lambda i, t: t + gslots[g, i], grads[g, mine_now])

            def send(i, carry):
                to_all(g, part, lax.rem(flat + i, count)).start()
                return carry

            lax.fori_loop(1, count, send, 0)

    def reduce_end(g):
        @pl.when(is_owner(g))
        def _():
            others = pl.ds(0, chunks - per)
            whole_copy(done.at[g, others], back_out.at[g], back_in.at[g]).wait_recv()
            whole_copy(grads.at[g, others], red_out.at[g], red_in.at[g]).wait_send()
            whole_copy(gslots.at[g], back_out.at[g], back_in.at[g]).wait_send()

        @pl.when(jnp.logical_not(is_owner(g)))
        def _():
            whole_copy(done.at[g], back_out.at[g], back_in.at[g]).wait_recv()
            whole_copy(grads.at[g], red_out.at[g], red_in.at[g]).wait_send()

        for i in range(per_group):
            sums_ref[g * per_group + i] = done[g, i]
            sums_ref[heads + g * per_group + i] = done[g, per_group + i]

    put_out = pltpu.make_async_copy(qin, out_ref, out_sem)

    def write_out(n):
        qin[at(n)] = by_head(oh[:, at(n)])

    with jax.named_scope("write_out"):
        for n in range(1, tiles):
            write_out(n)

    def first_keys(hs):
        kept = kept_part(hs, 0, key_features(hs, [0]))
        weight = weights(hs, 1)
        for i, h in enumerate(hs):
            fkept[h] = kept[i]
            prob[h] = weight[i]

    def first_values(hs):
        flip_values(hs, [0])
        kept = [fkept[h] for h in hs]
        state = [split_dot(dot_nn, k, vx[h, at(0)]) for k, h in zip(kept, hs)]
        for i, h in enumerate(hs):
            skept[0, h] = state[i]
            nkept[0, h] = spread(kept[i])
        weighted(hs, 1, [prob[h] for h in hs])
        combine(hs, 1)

    for g in range(GROUPS):
        first, last = g * per_group, (g + 1) * per_group
        with jax.named_scope("halo_k"):
            halo_wait(g, 0)
        with jax.named_scope("first_keys"):
            kx[first:last, at(0)] = by_head(halo[g, 0])
            over_heads(first, last, UNROLL, first_keys)
        with jax.named_scope("halo_v"):
            halo_wait(g, 1)
        with jax.named_scope("first_values"):
            vx[first:last, at(0)] = by_head(halo[g, 1])
            over_heads(first, last, UNROLL, first_values)
        with jax.named_scope("send_ds"):
            message_start(g)
        with jax.named_scope("local_keys"):
            over_heads(first, last, UNROLL, local_keys)
    with jax.named_scope("write_0"):
        write_out(0)
        put_out.start()
    for g in range(GROUPS):
        with jax.named_scope("wait_ds"):
            message_sum(g)
        with jax.named_scope("final_keys"):
            over_heads(g * per_group, (g + 1) * per_group, UNROLL, final_keys)
        with jax.named_scope("red_start"):
            reduce_start(g)
    with jax.named_scope("red_own"):
        for g in range(GROUPS):
            reduce_own(g)
    with jax.named_scope("red_end"):
        for g in range(GROUPS):
            reduce_end(g)
    with jax.named_scope("sent"):
        @pl.when(me < peers - 1)
        def _():
            whole_copy(halo, halo_out, halo_in.at[0, 0]).wait_send()

        states_sent()
        for g in range(GROUPS):
            message_sent(g)
        put_out.wait()


def finish_kernel(rows_hbm, sums_hbm, out_hbm, gq_hbm, gk_hbm, rows, sums, in_sem, out_sem):
    tokens = rows.shape[0]
    heads = gq_hbm.shape[0]
    parts = [pl.ds(i * heads, heads) for i in range(2)]
    sums_in = pltpu.make_async_copy(sums_hbm, sums, in_sem.at[PIECES])
    chunks = [pl.ds(i * (tokens // PIECES), tokens // PIECES) for i in range(PIECES)]
    rows_in = [pltpu.make_async_copy(rows_hbm.at[c], rows.at[c], in_sem.at[i]) for i, c in enumerate(chunks)]
    rows_out = [pltpu.make_async_copy(rows.at[c], out_hbm.at[c], out_sem.at[i]) for i, c in enumerate(chunks)]
    outs = [(sums.at[parts[0]], gq_hbm), (sums.at[parts[1]], gk_hbm)]
    sums_out = [pltpu.make_async_copy(a, b, out_sem.at[PIECES + i]) for i, (a, b) in enumerate(outs)]
    sums_in.start()
    for copy in rows_in:
        copy.start()
    sums_in.wait()
    for copy in sums_out:
        copy.start()
    for i in range(PIECES):
        rows_in[i].wait()
        rows_out[i].start()
    for copy in sums_out + rows_out:
        copy.wait()


def body(queries, keys, values, keep_count, query_map, key_map, cotangent):
    q_rows, k_rows, v_rows, cot = queries[0], keys[0], values[0], cotangent[0]
    tokens, heads, width = q_rows.shape
    rank = query_map.shape[2]
    tiles = tokens // TILE
    axes = ("seq", "batch")
    peers = lax.axis_size("seq")
    count = peers * lax.axis_size("batch")
    per_group = heads // GROUPS
    chunks = 2 * per_group
    owners, per = owners_of(count, chunks)
    block = (per_group + 2, rank, width)
    hbm = pl.BlockSpec(memory_space=pltpu.HBM)
    vmem = pl.BlockSpec(memory_space=pltpu.VMEM)
    dma = pltpu.SemaphoreType.DMA
    small = pltpu.VMEM((heads, rank, width), F32)
    tiled = pltpu.VMEM((tiles + 1, heads, rank, width), F32)
    states = (heads + 2, rank, width)
    packed = pltpu.VMEM((heads, rank, width), BF16)
    operands = [q_rows, k_rows, v_rows, cot, jnp.swapaxes(query_map, 1, 2), jnp.swapaxes(key_map, 1, 2)]
    rows, sums = pl.pallas_call(
        functools.partial(layer_kernel, "seq", axes),
        name="layer",
        in_specs=[hbm] * 7,
        out_specs=[hbm, vmem],
        out_shape=[
            jax.ShapeDtypeStruct((tokens, heads, width), BF16),
            jax.ShapeDtypeStruct((2 * heads, rank, width), F32),
        ],
        scratch_shapes=[pltpu.VMEM((tokens, heads, width), BF16)] * 4
        + [pltpu.VMEM((heads, tokens + TILE, width), BF16)] * 2
        + [
            pltpu.VMEM((heads, width, tokens + TILE), BF16),
            pltpu.VMEM((heads, tokens, width), BF16),
            pltpu.VMEM((heads, width, tokens), BF16),
            pltpu.VMEM((heads, tokens, width), BF16),
            pltpu.VMEM((GROUPS, 2, TILE, per_group, width), BF16),
            pltpu.VMEM((heads, width, tokens), F32),
            pltpu.VMEM((heads, 8, tokens), F32),
            pltpu.VMEM((heads, rank, tokens), F32),
            pltpu.VMEM((heads, rank, tokens + TILE), F32),
            tiled, tiled, tiled, tiled, small, small, tiled, tiled, small, small,
            pltpu.SMEM(keep_count.shape[1:], jnp.int32),
            packed, packed,
            pltpu.VMEM((heads, 2 * TILE, TILE), BF16),
            small,
            pltpu.VMEM(states, F32),
            pltpu.VMEM((3,) + states, BF16),
            pltpu.VMEM((2,) + states, BF16),
            pltpu.VMEM((peers // 2,) + states, BF16),
            pltpu.VMEM((GROUPS,) + block, BF16),
            pltpu.VMEM((GROUPS, peers) + block, BF16),
            pltpu.VMEM((GROUPS, chunks, rank, width), F32),
            pltpu.VMEM((GROUPS, count - 1, per, rank, width), F32),
            pltpu.VMEM((GROUPS, chunks, rank, width), F32),
            dma((4,)), dma((3,)), dma(()), dma((GROUPS, 2)), dma((2,)), dma((2,)),
            dma((peers // 2,)), dma((peers // 2,)), dma((GROUPS, peers)), dma((GROUPS, peers)),
            dma((GROUPS,)), dma((GROUPS,)), dma((GROUPS,)), dma((GROUPS,)), dma(()),
        ],
        compiler_params=pltpu.CompilerParams(
            collective_id=0, has_side_effects=True, vmem_limit_bytes=VMEM_LIMIT
        ),
    )(keep_count[0], *operands)
    out, gq, gk = pl.pallas_call(
        finish_kernel,
        name="finish",
        in_specs=[hbm, hbm],
        out_specs=[hbm, hbm, hbm],
        out_shape=[
            jax.ShapeDtypeStruct((tokens, heads, width), BF16),
            jax.ShapeDtypeStruct((heads, rank, width), F32),
            jax.ShapeDtypeStruct((heads, rank, width), F32),
        ],
        scratch_shapes=[
            pltpu.VMEM((tokens, heads, width), BF16),
            pltpu.VMEM((2 * heads, rank, width), F32),
            dma((PIECES + 1,)), dma((PIECES + 2,)),
        ],
        compiler_params=pltpu.CompilerParams(vmem_limit_bytes=VMEM_LIMIT),
    )(rows, sums)
    return out[None], jnp.swapaxes(gq, 1, 2), jnp.swapaxes(gk, 1, 2)


def solution(mesh):
    placed = (
        P("batch", "seq", None, None),
        P("batch", "seq", None, None),
        P("batch", "seq", None, None),
        P("batch", None, None),
        P(),
        P(),
        P("batch", "seq", None, None),
    )
    return jax.shard_map(
        body,
        mesh=mesh,
        in_specs=placed,
        out_specs=(P("batch", "seq", None, None), P(), P()),
        check_vma=False,
    )
```

```python
import functools
import math

import jax
import jax.numpy as jnp
from jax import lax
from jax.experimental import pallas as pl
from jax.experimental.pallas import tpu as pltpu
from jax.sharding import PartitionSpec as P

TILE = 128
SHIFT = 1.5
LOG2E = 1.0 / math.log(2.0)
MASKED = -1e30
F32 = jnp.float32
BF16 = jnp.bfloat16
GROUPS = 2
UNROLL = 4
CUTS = 4
EARLY_EVEN = 9
EARLY_ODD = 3
LATE = 8
PARTS = 4
VMEM_LIMIT = 50 * 1024 * 1024


def dot_nt(a, b):
    return lax.dot_general(a, b, (((1,), (1,)), ((), ())), preferred_element_type=F32)


def dot_nn(a, b):
    return lax.dot_general(a, b, (((1,), (0,)), ((), ())), preferred_element_type=F32)


def dot_tn(a, b):
    return lax.dot_general(a, b, (((0,), (0,)), ((), ())), preferred_element_type=F32)


def by_head(x):
    return jnp.swapaxes(x, 0, 1)


def softplus(x):
    return jnp.maximum(x, 0.0) + jnp.log1p(jnp.exp(-jnp.abs(x)))


def sigmoid(x):
    return 1.0 / (1.0 + jnp.exp(-x))


def halves(x):
    top = x.astype(BF16)
    return top, (x - top.astype(F32)).astype(BF16)


def split_dot(dot, x, y):
    rows = x.shape[0]
    both = dot(jnp.concatenate(halves(x), 0), y)
    return both[:rows] + both[rows:]


def flat_id(axes):
    index, count = 0, 1
    for axis in axes:
        index = index * lax.axis_size(axis) + lax.axis_index(axis)
        count *= lax.axis_size(axis)
    return index, count


def place(flat, axes):
    where = {}
    for axis in reversed(axes):
        size = lax.axis_size(axis)
        where[axis] = lax.rem(flat, size)
        flat = flat // size
    return where


def each_other(axes, act):
    outer, inner = axes
    me, mine = lax.axis_index(outer), lax.axis_index(inner)
    peers, others = lax.axis_size(outer), lax.axis_size(inner)

    def far(i, carry):
        s = me + i
        s = jnp.where(s >= peers, s - peers, s)
        for b in range(others):
            act({outer: s, inner: b})
        return carry

    lax.fori_loop(1, peers, far, 0)
    for b in range(others):

        @pl.when(mine != b)
        def _(b=b):
            act({outer: me, inner: b})


def greet(axes):
    barrier = pltpu.get_barrier_semaphore()
    each_other(
        axes,
        lambda where: pl.semaphore_signal(barrier, inc=1, device_id=where, device_id_type=pl.DeviceIdType.MESH),
    )
    return barrier


def at(tile, count=1):
    return pl.ds(tile * TILE, count * TILE)


def owners_of(count, chunks):
    owners = min(count, chunks)
    stride = 2 if count >= 2 * owners else 1
    return owners, stride, (count - owners * stride) // 2 + stride - 1


def layer_kernel(
    seq, axes, counts_hbm, q_hbm, k_hbm, v_hbm, c_hbm, wq_hbm, wk_hbm, out_ref, sums_ref,
    qin, kin, vin, cin, kx, vx, vt, qx, ct, oh, halo, num, rows, preq, sigk, sall, nall, skept, nkept,
    sin, nin, dsb, dnb, gaf, naf, counts_ref, wq_ref, wk_ref, prob, fkept, sent_halo,
    own, state_out, state_in, even_in, mine, slots, grads, qslots, kslots, done,
    in_sem, edge_sem, small_sem, halo_out, halo_in, pair_out, pair_in, even_out_sem, even_in_sem,
    msg_out, msg_in, red_out, red_in, back_out, back_in,
):
    tokens, heads, width = q_hbm.shape
    rank = wq_hbm.shape[1]
    tiles = tokens // TILE
    per_group = heads // GROUPS
    factor = LOG2E / math.sqrt(width)
    me = lax.axis_index(seq)
    peers = lax.axis_size(seq)
    flat, count = flat_id(axes)
    sq = (seq,)
    barrier = greet(axes)
    base = me * tiles
    lane = lax.broadcasted_iota(jnp.int32, (1, TILE), 1)
    sub = lax.broadcasted_iota(jnp.int32, (TILE, TILE), 0)
    causal = sub <= lax.broadcasted_iota(jnp.int32, (TILE, TILE), 1)

    early = [
        pltpu.make_async_copy(
            hbm.at[pl.ds(tokens - TILE, TILE), pl.ds(g * per_group, per_group)], sent_halo.at[g, i], edge_sem.at[g, i]
        )
        for g in range(GROUPS)
        for i, hbm in enumerate((k_hbm, v_hbm))
    ]
    for copy in early:
        copy.start()
    pairs_in = [(k_hbm, kin), (v_hbm, vin), (q_hbm, qin), (c_hbm, cin)]
    loads = [pltpu.make_async_copy(hbm, vmem, in_sem.at[i]) for i, (hbm, vmem) in enumerate(pairs_in)]
    for copy in loads:
        copy.start()

    smalls = [
        pltpu.make_async_copy(counts_hbm, counts_ref, small_sem.at[0]),
        pltpu.make_async_copy(wk_hbm, wk_ref, small_sem.at[1]),
        pltpu.make_async_copy(wq_hbm, wq_ref, small_sem.at[2]),
    ]
    for copy in smalls:
        copy.start()

    @pl.when(me == 0)
    def _():
        halo[...] = jnp.zeros_like(halo)
        state_in[0] = jnp.zeros_like(state_in[0])

    even = lax.rem(me, 2) == 0
    cut = TILE // CUTS
    pieces = [(g, i, r) for g in range(GROUPS) for i in range(2) for r in range(CUTS)]

    def halo_copy(g, i, r):
        return pltpu.make_async_remote_copy(
            src_ref=sent_halo.at[g, i, pl.ds(r * cut, cut)],
            dst_ref=halo.at[g, i, pl.ds(r * cut, cut)],
            send_sem=halo_out,
            recv_sem=halo_in.at[g, i],
            device_id=place(lax.rem(me + 1, peers), sq),
            device_id_type=pl.DeviceIdType.MESH,
        )

    def whole_copy(ref, send_sem, recv_sem):
        return pltpu.make_async_remote_copy(
            src_ref=ref,
            dst_ref=ref,
            send_sem=send_sem,
            recv_sem=recv_sem,
            device_id=place(lax.rem(me + 1, peers), sq),
            device_id_type=pl.DeviceIdType.MESH,
        )

    def halo_wait(g, i):
        @pl.when(me > 0)
        def _():
            whole_copy(halo.at[g, i], halo_out, halo_in.at[g, i]).wait_recv()

    for copy in early[:2]:
        copy.wait()
    with jax.named_scope("barrier"):
        pl.semaphore_wait(barrier, count - 1)

    def halo_start(mine, some):
        @pl.when(mine & (me < peers - 1))
        def _():
            for piece in some:
                halo_copy(*piece).start()

    odd = jnp.logical_not(even)
    first_group = 2 * CUTS
    halo_start(even, pieces[:first_group])
    halo_start(odd, pieces[:EARLY_ODD])
    for copy in early[2:]:
        copy.wait()
    halo_start(even, pieces[first_group:EARLY_EVEN])

    def count_before(h, e):
        if e:
            return counts_ref[h, base + e - 1]
        return jnp.where(me > 0, counts_ref[h, jnp.maximum(base - 1, 0)], 0)

    def pair_copy(i, target):
        return pltpu.make_async_remote_copy(
            src_ref=state_out.at[i],
            dst_ref=state_in.at[i],
            send_sem=pair_out.at[i],
            recv_sem=pair_in.at[i],
            device_id=place(target, sq),
            device_id_type=pl.DeviceIdType.MESH,
        )

    def even_copy(sender, target):
        return pltpu.make_async_remote_copy(
            src_ref=state_out.at[2],
            dst_ref=even_in.at[sender],
            send_sem=even_out_sem.at[target],
            recv_sem=even_in_sem.at[sender],
            device_id=place(2 * target, sq),
            device_id_type=pl.DeviceIdType.MESH,
        )

    def pack(i, total):
        state_out[i, :heads] = total[:heads].astype(BF16)
        state_out[i, heads], state_out[i, heads + 1] = halves(total[heads] + total[heads + 1])

    def set_states(total):
        norms = total[heads] + total[heads + 1]
        for h in range(heads):
            sin[h] = total[h]
            nin[h] = spread(jnp.where(lane == h, norms, 0.0))

    pair, pairs = me // 2, peers // 2

    def own_states():
        packed = jnp.zeros((rank, width), F32)
        for h in range(heads):
            own[h] = sum(sall[e, h] for e in ext)
            packed = jnp.where(lane == h, sum(nall[e, h] for e in ext), packed)
        own[heads] = packed
        own[heads + 1] = jnp.zeros((rank, width), F32)

        @pl.when(odd & (me < peers - 1))
        def _():
            pack(0, own[...])
            pair_copy(0, me + 1).start()

        halo_start(odd, pieces[EARLY_ODD:])

    def pair_states():
        @pl.when(even)
        def _():
            @pl.when(me > 0)
            def _():
                pair_copy(0, me + 1).wait_recv()

            pack(2, own[...] + state_in[0].astype(F32))

            def send(p, carry):
                even_copy(pair, p).start()
                return carry

            lax.fori_loop(pair + 1, pairs, send, 0)

    def even_states():
        @pl.when(even)
        def _():
            def received(p, total):
                even_copy(p, lax.rem(pair + 1, pairs)).wait_recv()
                return total + even_in[p].astype(F32)

            total = lax.fori_loop(0, pair, received, state_in[0].astype(F32))
            pack(1, own[...] + total)
            pair_copy(1, me + 1).start()

            halo_start(even, pieces[EARLY_EVEN:])
            set_states(total)

    def odd_states():
        @pl.when(odd)
        def _():
            pair_copy(1, me - 1).wait_recv()
            set_states(state_in[1].astype(F32))

    def states_sent():
        @pl.when(even)
        def _():
            def sent(p, carry):
                even_copy(pair, p).wait_send()
                return carry

            lax.fori_loop(pair + 1, pairs, sent, 0)
            pair_copy(1, me + 1).wait_send()

        @pl.when(odd & (me < peers - 1))
        def _():
            pair_copy(0, me + 1).wait_send()

    def message(g, sender, target):
        return pltpu.make_async_remote_copy(
            src_ref=mine.at[g],
            dst_ref=slots.at[g, sender],
            send_sem=msg_out.at[g, target],
            recv_sem=msg_in.at[g, sender],
            device_id=place(target, sq),
            device_id_type=pl.DeviceIdType.MESH,
        )

    def message_start(g):
        every = range(1, tiles + 1)
        packed = jnp.zeros((rank, width), F32)
        for i in range(per_group):
            h = g * per_group + i
            mine[g, i] = sum(dsb[j, h] for j in every).astype(BF16)
            packed = jnp.where(lane == i, sum(dnb[j, h] for j in every), packed)
        mine[g, per_group], mine[g, per_group + 1] = halves(packed)

        def send(p, carry):
            message(g, me, p).start()
            return carry

        lax.fori_loop(0, me, send, 0)

    def message_sent(g):
        def sent(p, carry):
            message(g, me, p).wait_send()
            return carry

        lax.fori_loop(0, me, sent, 0)

    def message_sum(g):
        def received(p, total):
            message(g, p, lax.rem(me + 1, peers)).wait_recv()
            return total + slots[g, p].astype(F32)

        total = lax.fori_loop(me + 1, peers, received, jnp.zeros((per_group + 2, rank, width), F32))
        norms = total[per_group] + total[per_group + 1]
        for i in range(per_group):
            gaf[g * per_group + i] = total[i]
            naf[g * per_group + i] = spread(jnp.where(lane == i, norms, 0.0))

    def spread(x):
        return jnp.broadcast_to(jnp.sum(x, 1, keepdims=True), (rank, width))

    def over_heads(first, last, step, act):
        def block(i, carry):
            act([first + i * step + u for u in range(step)])
            return carry

        lax.fori_loop(0, (last - first) // step, block, 0)

    ext = list(range(1, tiles + 1))
    with jax.named_scope("keys"):
        loads[0].wait()
        for n in range(tiles):
            kx[:, at(n + 1)] = by_head(kin[at(n)])
    with jax.named_scope("values"):
        loads[1].wait()
        for n in range(tiles):
            vx[:, at(n + 1)] = by_head(vin[at(n)])
    with jax.named_scope("maps"):
        for copy in smalls:
            copy.wait()

    def key_features(hs, tile_list):
        where = at(tile_list[0], len(tile_list))
        pre = [dot_nt(wk_ref[h], kx[h, where]) - SHIFT for h in hs]
        for h, p in zip(hs, pre):
            sigk[h, :, where] = sigmoid(p)
        return [softplus(p) for p in pre]

    def kept_part(hs, e, feat):
        return [f * (lane < count_before(h, e)).astype(F32) for f, h in zip(feat, hs)]

    def key_states(hs):
        feat = key_features(hs, ext)
        for e in ext:
            one = [f[:, (e - 1) * TILE : e * TILE] for f in feat]
            if e < tiles:
                kept = kept_part(hs, e, one)
                both = [split_dot(dot_nn, jnp.concatenate([o, k], 0), vx[h, at(e)]) for o, k, h in zip(one, kept, hs)]
                for i, h in enumerate(hs):
                    skept[e, h] = both[i][rank:]
                    nkept[e, h] = spread(kept[i])
            else:
                both = [split_dot(dot_nn, o, vx[h, at(e)]) for o, h in zip(one, hs)]
            for i, h in enumerate(hs):
                sall[e, h] = both[i][:rank]
                nall[e, h] = spread(one[i])

    with jax.named_scope("states"):
        over_heads(0, heads, UNROLL, key_states)
        own_states()

    def flip_values(hs, tile_list):
        for h in hs:
            for e in tile_list:
                vt[h, :, at(e)] = vx[h, at(e)].T

    with jax.named_scope("flip_v"):
        over_heads(0, heads, UNROLL, lambda hs: flip_values(hs, ext))
    with jax.named_scope("queries"):
        loads[2].wait()
        for n in range(tiles):
            qx[:, at(n)] = by_head(qin[at(n)])

    def query_features(hs):
        pre = [dot_nt(wq_ref[h], qx[h]) - SHIFT for h in hs]
        for h, p in zip(hs, pre):
            preq[h] = p

    with jax.named_scope("qfeat"):
        over_heads(0, heads, UNROLL, query_features)
    def weights(hs, j):
        each = range(len(hs))
        scores = [dot_nt(kx[h, at(j - 1, 2)], qx[h, at(j - 1)]) for h in hs]
        old = [jnp.where(sub < count_before(h, j - 1), scores[i][:TILE], MASKED) for i, h in enumerate(hs)]
        new = [jnp.where(causal, scores[i][TILE:], MASKED) for i in each]
        top = [jnp.max(jnp.maximum(old[i], new[i]), 0, keepdims=True) * factor for i in each]
        old = [jnp.exp2(old[i] * factor - top[i]) for i in each]
        new = [jnp.exp2(new[i] * factor - top[i]) for i in each]
        for i, h in enumerate(hs):
            rows[h, 0:1, at(j - 1)] = jnp.sum(old[i] + new[i], 0, keepdims=True)
            rows[h, 1:2, at(j - 1)] = top[i]
        return [jnp.concatenate([old[i].astype(BF16), new[i].astype(BF16)], 0) for i in each]

    def weighted(hs, j, weight):
        numer = [dot_nn(vt[h, :, at(j - 1, 2)], w) for h, w in zip(hs, weight)]
        for h, x in zip(hs, numer):
            num[h, :, at(j - 1)] = x

    def sparse(hs, j):
        weighted(hs, j, weights(hs, j))

    with jax.named_scope("sparse"):
        for j in range(2, tiles + 1):
            over_heads(0, heads, UNROLL, lambda hs, j=j: sparse(hs, j))
            if j == 2:
                with jax.named_scope("pair_states"):
                    pair_states()
    with jax.named_scope("even_states"):
        even_states()
    with jax.named_scope("cot"):
        loads[3].wait()
        for n in range(tiles):
            oh[:, at(n)] = by_head(cin[at(n)])

    def flip_cotangent(hs):
        for h in hs:
            for n in range(tiles):
                ct[h, :, at(n)] = oh[h, at(n)].T

    with jax.named_scope("flip_c"):
        over_heads(0, heads, UNROLL, flip_cotangent)
    with jax.named_scope("odd_states"):
        odd_states()

    def combine(hs, j):
        each = range(len(hs))
        where = at(j - 1)
        pre = [preq[h, :, where] for h in hs]
        feat = [softplus(p) for p in pre]
        state = [sum([sall[e, h] for e in range(1, j)], sin[h]) - skept[j - 1, h] for h in hs]
        norm = [sum([nall[e, h] for e in range(1, j)], nin[h]) - nkept[j - 1, h] for h in hs]
        decay = [jnp.exp2(-rows[h, 1:2, where]) for h in hs]
        kernel = []
        for i in each:
            fq_top, fq_low = halves(feat[i])
            st_top, st_low = halves(state[i])
            kernel.append(
                dot_tn(jnp.concatenate([st_top, st_top, st_low], 0), jnp.concatenate([fq_top, fq_low, fq_top], 0))
            )
        den = [jnp.sum(norm[i] * feat[i], 0, keepdims=True) for i in each]
        inv = [1.0 / (rows[h, 0:1, where] + decay[i] * den[i]) for i, h in enumerate(hs)]
        out = [(num[h, :, where] + decay[i] * kernel[i]) * inv[i] for i, h in enumerate(hs)]
        grad = [ct[h, :, where].astype(F32) * (decay[i] * inv[i]) for i, h in enumerate(hs)]
        dot = [jnp.sum(grad[i] * out[i], 0, keepdims=True) for i in each]
        grad = [x.astype(BF16) for x in grad]
        for i, h in enumerate(hs):
            oh[h, where] = out[i].astype(BF16).T
        d_fq = [split_dot(dot_nn, state[i], grad[i]) - norm[i] * dot[i] for i in each]
        ds = [split_dot(dot_nt, feat[i], grad[i]) for i in each]
        gq = [split_dot(dot_nn, d_fq[i] * sigmoid(pre[i]), qx[h, where]) for i, h in enumerate(hs)]
        for i, h in enumerate(hs):
            dsb[j, h] = ds[i]
            dnb[j, h] = -spread(feat[i] * dot[i])
            if j == tiles:
                grads[h] = gq[i]
            else:
                grads[h] += gq[i]

    with jax.named_scope("combine"):
        for j in range(tiles, 1, -1):
            over_heads(0, heads, UNROLL, lambda hs, j=j: combine(hs, j))

    def local_keys(hs):
        parts = [[] for _ in hs]
        for e in range(tiles):
            later = None
            if 0 < e < tiles - 1:
                later = [sum(dsb[j, h] for j in range(e + 2, tiles + 1)) for h in hs]
            near = [dsb[e + 1, h] for h in hs]
            kept = [(lane < count_before(h, e)).astype(F32) for h in hs]
            for i, h in enumerate(hs):
                values = vt[h, :, at(e)]
                if e == 0:
                    part = -kept[i] * (split_dot(dot_nn, near[i], values) + dnb[1, h])
                elif later is None:
                    part = (1.0 - kept[i]) * (split_dot(dot_nn, near[i], values) + dnb[e + 1, h])
                else:
                    both = split_dot(dot_nn, jnp.concatenate([near[i], later[i]], 0), values)
                    far = both[rank:] + sum(dnb[j, h] for j in range(e + 2, tiles + 1))
                    part = (1.0 - kept[i]) * (both[:rank] + dnb[e + 1, h]) + far
                parts[i].append(part * sigk[h, :, at(e)])
        for i, h in enumerate(hs):
            grads[heads + h] = split_dot(dot_nn, jnp.concatenate(parts[i], 1), kx[h, at(0, tiles)])

    def final_keys(hs):
        own = at(1, tiles)
        d_fk = [split_dot(dot_nn, gaf[h], vt[h, :, own]) + naf[h][:, :1] for h in hs]
        gk = [split_dot(dot_nn, d_fk[i] * sigk[h, :, own], kx[h, own]) for i, h in enumerate(hs)]
        for i, h in enumerate(hs):
            grads[heads + h] += gk[i]

    owners, stride, middle = owners_of(count, per_group)
    rounds = [(0, heads)] + [(heads + g * per_group, per_group) for g in range(GROUPS)]
    ahead = flat - middle + count * stride
    part = lax.rem(ahead // stride, owners)
    inside = (flat >= middle) & (flat < middle + owners * stride) & (lax.rem(ahead, stride) == 0)

    def share(r, o):
        first, size = rounds[r]
        per = size // owners
        return pl.ds(first + o * per, per)

    def arriving(r):
        return kslots.at[r - 1] if r else qslots

    def to_owner(r, o):
        target = middle + o * stride
        return pltpu.make_async_remote_copy(
            src_ref=grads.at[share(r, o)],
            dst_ref=arriving(r).at[lax.rem(flat - target + count - 1, count)],
            send_sem=red_out.at[r],
            recv_sem=red_in.at[r],
            device_id=dict(zip(axes, divmod(target, lax.axis_size(axes[1])))),
            device_id_type=pl.DeviceIdType.MESH,
        )

    def to_all(r, where):
        return pltpu.make_async_remote_copy(
            src_ref=done.at[share(r, part)],
            dst_ref=done.at[share(r, part)],
            send_sem=back_out.at[r],
            recv_sem=back_in.at[r],
            device_id=where,
            device_id_type=pl.DeviceIdType.MESH,
        )

    def reduce_start(r):
        for o in range(owners):

            @pl.when(middle + o * stride != flat)
            def _(o=o):
                to_owner(r, o).start()

    def reduce_own(r):
        @pl.when(inside)
        def _():
            slots_now = arriving(r)
            whole_copy(slots_now, red_out.at[r], red_in.at[r]).wait_recv()
            done[share(r, part)] = grads[share(r, part)] + jnp.sum(slots_now[...], 0)
            each_other(axes, lambda where: to_all(r, where).start())

    def reduce_end(r):
        first, size = rounds[r]
        per = size // owners
        every, others = pl.ds(first, size), pl.ds(first, size - per)

        @pl.when(inside)
        def _():
            if owners > 1:
                whole_copy(done.at[others], back_out.at[r], back_in.at[r]).wait_recv()
                whole_copy(grads.at[others], red_out.at[r], red_in.at[r]).wait_send()
            whole_copy(arriving(r), back_out.at[r], back_in.at[r]).wait_send()

        @pl.when(jnp.logical_not(inside))
        def _():
            whole_copy(done.at[every], back_out.at[r], back_in.at[r]).wait_recv()
            whole_copy(grads.at[every], red_out.at[r], red_in.at[r]).wait_send()

        sums_ref[every] = done[every]

    def write_out(n):
        out_ref[at(n)] = by_head(oh[:, at(n)])

    with jax.named_scope("write_out"):
        for n in range(1, tiles):
            write_out(n)

    def first_keys(hs):
        kept = kept_part(hs, 0, key_features(hs, [0]))
        weight = weights(hs, 1)
        for i, h in enumerate(hs):
            fkept[h] = kept[i]
            prob[h] = weight[i]

    def first_values(hs):
        flip_values(hs, [0])
        kept = [fkept[h] for h in hs]
        state = [split_dot(dot_nn, k, vx[h, at(0)]) for k, h in zip(kept, hs)]
        for i, h in enumerate(hs):
            skept[0, h] = state[i]
            nkept[0, h] = spread(kept[i])
        weighted(hs, 1, [prob[h] for h in hs])
        combine(hs, 1)

    for g in range(GROUPS):
        first, last = g * per_group, (g + 1) * per_group
        with jax.named_scope("halo_k"):
            halo_wait(g, 0)
        with jax.named_scope("first_keys"):
            kx[first:last, at(0)] = by_head(halo[g, 0])
            over_heads(first, last, LATE, first_keys)
        with jax.named_scope("halo_v"):
            halo_wait(g, 1)
        with jax.named_scope("first_values"):
            vx[first:last, at(0)] = by_head(halo[g, 1])
            over_heads(first, last, LATE, first_values)
        with jax.named_scope("send_ds"):
            message_start(g)
        with jax.named_scope("local_keys"):
            over_heads(first, last, UNROLL, local_keys)
    with jax.named_scope("write_0"):
        write_out(0)
    reduce_start(0)
    for g in range(GROUPS):
        with jax.named_scope("wait_ds"):
            message_sum(g)
        with jax.named_scope("final_keys"):
            over_heads(g * per_group, (g + 1) * per_group, LATE, final_keys)
        with jax.named_scope("red_start"):
            reduce_start(1 + g)
    with jax.named_scope("red_own"):
        for r in range(1 + GROUPS):
            reduce_own(r)
    with jax.named_scope("red_end"):
        for r in range(1 + GROUPS):
            reduce_end(r)
    with jax.named_scope("sent"):
        @pl.when(me < peers - 1)
        def _():
            whole_copy(halo, halo_out, halo_in.at[0, 0]).wait_send()

        states_sent()
        for g in range(GROUPS):
            message_sent(g)


def finish_kernel(rows_ref, sums_ref, out_hbm, gq_hbm, gk_hbm, sem):
    heads = gq_hbm.shape[0]
    tokens = rows_ref.shape[0] // PARTS
    copies = [
        pltpu.make_async_copy(sums_ref.at[pl.ds(0, heads)], gq_hbm, sem.at[PARTS]),
        pltpu.make_async_copy(sums_ref.at[pl.ds(heads, heads)], gk_hbm, sem.at[PARTS + 1]),
    ]
    for i in range(PARTS):
        some = pl.ds(i * tokens, tokens)
        copies.append(pltpu.make_async_copy(rows_ref.at[some], out_hbm.at[some], sem.at[i]))
    for copy in copies:
        copy.start()
    for copy in copies:
        copy.wait()


def body(queries, keys, values, keep_count, query_map, key_map, cotangent):
    q_rows, k_rows, v_rows, cot = queries[0], keys[0], values[0], cotangent[0]
    tokens, heads, width = q_rows.shape
    rank = query_map.shape[2]
    tiles = tokens // TILE
    axes = ("seq", "batch")
    peers = lax.axis_size("seq")
    count = peers * lax.axis_size("batch")
    per_group = heads // GROUPS
    owners, _, _ = owners_of(count, per_group)
    block = (per_group + 2, rank, width)
    hbm = pl.BlockSpec(memory_space=pltpu.HBM)
    vmem = pl.BlockSpec(memory_space=pltpu.VMEM)
    dma = pltpu.SemaphoreType.DMA
    small = pltpu.VMEM((heads, rank, width), F32)
    tiled = pltpu.VMEM((tiles + 1, heads, rank, width), F32)
    states = (heads + 2, rank, width)
    packed = pltpu.VMEM((heads, rank, width), BF16)
    operands = [keep_count[0], q_rows, k_rows, v_rows, cot, jnp.swapaxes(query_map, 1, 2), jnp.swapaxes(key_map, 1, 2)]
    rows, sums = pl.pallas_call(
        functools.partial(layer_kernel, "seq", axes),
        name="layer",
        in_specs=[hbm] * 7,
        out_specs=[vmem, vmem],
        out_shape=[
            jax.ShapeDtypeStruct((tokens, heads, width), BF16),
            jax.ShapeDtypeStruct((2 * heads, rank, width), F32),
        ],
        scratch_shapes=[pltpu.VMEM((tokens, heads, width), BF16)] * 4
        + [pltpu.VMEM((heads, tokens + TILE, width), BF16)] * 2
        + [
            pltpu.VMEM((heads, width, tokens + TILE), BF16),
            pltpu.VMEM((heads, tokens, width), BF16),
            pltpu.VMEM((heads, width, tokens), BF16),
            pltpu.VMEM((heads, tokens, width), BF16),
            pltpu.VMEM((GROUPS, 2, TILE, per_group, width), BF16),
            pltpu.VMEM((heads, width, tokens), F32),
            pltpu.VMEM((heads, 8, tokens), F32),
            pltpu.VMEM((heads, rank, tokens), F32),
            pltpu.VMEM((heads, rank, tokens + TILE), F32),
            tiled, tiled, tiled, tiled, small, small, tiled, tiled, small, small,
            pltpu.SMEM(keep_count.shape[1:], jnp.int32),
            packed, packed,
            pltpu.VMEM((heads, 2 * TILE, TILE), BF16),
            small,
            pltpu.VMEM((GROUPS, 2, TILE, per_group, width), BF16),
            pltpu.VMEM(states, F32),
            pltpu.VMEM((3,) + states, BF16),
            pltpu.VMEM((2,) + states, BF16),
            pltpu.VMEM((peers // 2,) + states, BF16),
            pltpu.VMEM((GROUPS,) + block, BF16),
            pltpu.VMEM((GROUPS, peers) + block, BF16),
            pltpu.VMEM((2 * heads, rank, width), F32),
            pltpu.VMEM((count - 1, heads // owners, rank, width), F32),
            pltpu.VMEM((GROUPS, count - 1, per_group // owners, rank, width), F32),
            pltpu.VMEM((2 * heads, rank, width), F32),
            dma((4,)), dma((GROUPS, 2)), dma((3,)), dma(()), dma((GROUPS, 2)), dma((2,)), dma((2,)),
            dma((peers // 2,)), dma((peers // 2,)), dma((GROUPS, peers)), dma((GROUPS, peers)),
            dma((1 + GROUPS,)), dma((1 + GROUPS,)), dma((1 + GROUPS,)), dma((1 + GROUPS,)),
        ],
        compiler_params=pltpu.CompilerParams(
            collective_id=0, has_side_effects=True, vmem_limit_bytes=VMEM_LIMIT
        ),
    )(*[pltpu.with_memory_space_constraint(x, pltpu.HBM) for x in operands])
    out, gq, gk = pl.pallas_call(
        finish_kernel,
        name="finish",
        in_specs=[vmem, vmem],
        out_specs=[hbm, hbm, hbm],
        out_shape=[
            jax.ShapeDtypeStruct((tokens, heads, width), BF16),
            jax.ShapeDtypeStruct((heads, rank, width), F32),
            jax.ShapeDtypeStruct((heads, rank, width), F32),
        ],
        scratch_shapes=[dma((PARTS + 2,))],
        compiler_params=pltpu.CompilerParams(vmem_limit_bytes=VMEM_LIMIT),
    )(rows, sums)
    return out[None], jnp.swapaxes(gq, 1, 2), jnp.swapaxes(gk, 1, 2)


def solution(mesh):
    placed = (
        P("batch", "seq", None, None),
        P("batch", "seq", None, None),
        P("batch", "seq", None, None),
        P("batch", None, None),
        P(),
        P(),
        P("batch", "seq", None, None),
    )
    return jax.shard_map(
        body,
        mesh=mesh,
        in_specs=placed,
        out_specs=(P("batch", "seq", None, None), P(), P()),
        check_vma=False,
    )
```

```python
import functools
import math

import jax
import jax.numpy as jnp
from jax import lax
from jax.experimental import pallas as pl
from jax.experimental.pallas import tpu as pltpu
from jax.sharding import PartitionSpec as P

TILE = 128
SHIFT = 1.5
LOG2E = 1.0 / math.log(2.0)
MASKED = -1e30
F32 = jnp.float32
BF16 = jnp.bfloat16
UNROLL = 4
CUTS = 4
EARLY_EVEN = 9
EARLY_ODD = 3
PARTS = 4
VMEM_LIMIT = 50 * 1024 * 1024


def dot_nt(a, b):
    return lax.dot_general(a, b, (((1,), (1,)), ((), ())), preferred_element_type=F32)


def dot_nn(a, b):
    return lax.dot_general(a, b, (((1,), (0,)), ((), ())), preferred_element_type=F32)


def dot_tn(a, b):
    return lax.dot_general(a, b, (((0,), (0,)), ((), ())), preferred_element_type=F32)


def by_head(x):
    return jnp.swapaxes(x, 0, 1)


def softplus(x):
    return jnp.maximum(x, 0.0) + jnp.log1p(jnp.exp(-jnp.abs(x)))


def sigmoid(x):
    return 1.0 / (1.0 + jnp.exp(-x))


def halves(x):
    top = x.astype(BF16)
    return top, (x - top.astype(F32)).astype(BF16)


def split_dot(dot, x, y):
    rows = x.shape[0]
    both = dot(jnp.concatenate(halves(x), 0), y)
    return both[:rows] + both[rows:]


def flat_id(axes):
    index, count = 0, 1
    for axis in axes:
        index = index * lax.axis_size(axis) + lax.axis_index(axis)
        count *= lax.axis_size(axis)
    return index, count


def place(flat, axes):
    where = {}
    for axis in reversed(axes):
        size = lax.axis_size(axis)
        where[axis] = lax.rem(flat, size)
        flat = flat // size
    return where


def each_other(axes, act):
    outer, inner = axes
    me, mine = lax.axis_index(outer), lax.axis_index(inner)
    peers, others = lax.axis_size(outer), lax.axis_size(inner)

    def far(i, carry):
        s = me + i
        s = jnp.where(s >= peers, s - peers, s)
        for b in range(others):
            act({outer: s, inner: b})
        return carry

    lax.fori_loop(1, peers, far, 0)
    for b in range(others):

        @pl.when(mine != b)
        def _(b=b):
            act({outer: me, inner: b})


def greet(axes):
    barrier = pltpu.get_barrier_semaphore()
    each_other(
        axes,
        lambda where: pl.semaphore_signal(barrier, inc=1, device_id=where, device_id_type=pl.DeviceIdType.MESH),
    )
    return barrier


def at(tile, count=1):
    return pl.ds(tile * TILE, count * TILE)


def groups_of(heads):
    half, quarter = heads // 2, heads // 4
    return [(0, half), (half, quarter), (half + quarter, quarter)]


def owners_of(count, chunks):
    owners = min(count, chunks)
    stride = 2 if count >= 2 * owners else 1
    return owners, stride, (count - owners * stride) // 2 + stride - 1


def layer_kernel(
    seq, axes, counts_hbm, q_hbm, k_hbm, v_hbm, c_hbm, wq_hbm, wk_hbm, out_ref, sums_ref,
    qin, kin, vin, cin, kx, vx, vt, qx, ct, oh, halo, num, rows, preq, sigk, sall, nall, skept, nkept,
    sin, nin, dsb, dnb, gaf, naf, counts_ref, wq_ref, wk_ref, prob, fkept, sent_halo,
    own, state_out, state_in, even_in, mine, slots, grads, early_slots, late_slots, done,
    in_sem, edge_sem, small_sem, halo_out, halo_in, pair_out, pair_in, even_out_sem, even_in_sem,
    msg_out, msg_in, red_out, red_in, back_out, back_in,
):
    tokens, heads, width = q_hbm.shape
    rank = wq_hbm.shape[1]
    tiles = tokens // TILE
    groups = groups_of(heads)
    half = groups[0][1]
    factor = LOG2E / math.sqrt(width)
    me = lax.axis_index(seq)
    peers = lax.axis_size(seq)
    flat, count = flat_id(axes)
    sq = (seq,)
    barrier = greet(axes)
    base = me * tiles
    lane = lax.broadcasted_iota(jnp.int32, (1, TILE), 1)
    sub = lax.broadcasted_iota(jnp.int32, (TILE, TILE), 0)
    causal = sub <= lax.broadcasted_iota(jnp.int32, (TILE, TILE), 1)

    early = [
        pltpu.make_async_copy(
            hbm.at[pl.ds(tokens - TILE, TILE), pl.ds(0, half)], sent_halo.at[i], edge_sem.at[i]
        )
        for i, hbm in enumerate((k_hbm, v_hbm))
    ]
    for copy in early:
        copy.start()
    pairs_in = [(k_hbm, kin), (v_hbm, vin), (q_hbm, qin), (c_hbm, cin)]
    loads = [pltpu.make_async_copy(hbm, vmem, in_sem.at[i]) for i, (hbm, vmem) in enumerate(pairs_in)]
    for copy in loads:
        copy.start()

    smalls = [
        pltpu.make_async_copy(counts_hbm, counts_ref, small_sem.at[0]),
        pltpu.make_async_copy(wk_hbm, wk_ref, small_sem.at[1]),
        pltpu.make_async_copy(wq_hbm, wq_ref, small_sem.at[2]),
    ]
    for copy in smalls:
        copy.start()

    @pl.when(me == 0)
    def _():
        halo[...] = jnp.zeros_like(halo)
        blank = jnp.zeros((heads - half, TILE, width), BF16)
        kx[half:, at(0)] = blank
        vx[half:, at(0)] = blank
        state_in[0] = jnp.zeros_like(state_in[0])

    even = lax.rem(me, 2) == 0
    cut = TILE // CUTS
    pieces = [(0, i, r) for i in range(2) for r in range(CUTS)]
    for g, (first, size) in enumerate(groups[1:], 1):
        pieces += [(g, i, h) for i in range(2) for h in range(first, first + size, 2)]

    def halo_copy(g, i, r):
        if g:
            both = (kx, vx)[i].at[pl.ds(r, 2)]
            src, dst = both.at[:, at(tiles)], both.at[:, at(0)]
        else:
            src, dst = sent_halo.at[i, pl.ds(r * cut, cut)], halo.at[i, pl.ds(r * cut, cut)]
        return pltpu.make_async_remote_copy(
            src_ref=src,
            dst_ref=dst,
            send_sem=halo_out.at[1 + i if g else 0],
            recv_sem=halo_in.at[g, i],
            device_id=place(lax.rem(me + 1, peers), sq),
            device_id_type=pl.DeviceIdType.MESH,
        )

    def whole_copy(ref, send_sem, recv_sem):
        return pltpu.make_async_remote_copy(
            src_ref=ref,
            dst_ref=ref,
            send_sem=send_sem,
            recv_sem=recv_sem,
            device_id=place(lax.rem(me + 1, peers), sq),
            device_id_type=pl.DeviceIdType.MESH,
        )

    def halo_wait(g, i):
        @pl.when(me > 0)
        def _():
            landed = (kx, vx)[i].at[pl.ds(*groups[g]), at(0)] if g else halo.at[i]
            whole_copy(landed, halo_out.at[0], halo_in.at[g, i]).wait_recv()

    for copy in early:
        copy.wait()
    with jax.named_scope("barrier"):
        pl.semaphore_wait(barrier, count - 1)

    def halo_start(mine, some):
        @pl.when(mine & (me < peers - 1))
        def _():
            for piece in some:
                halo_copy(*piece).start()

    odd = jnp.logical_not(even)
    first_group = 2 * CUTS
    halo_start(even, pieces[:first_group])
    halo_start(odd, pieces[:EARLY_ODD])

    def count_before(h, e):
        if e:
            return counts_ref[h, base + e - 1]
        return jnp.where(me > 0, counts_ref[h, jnp.maximum(base - 1, 0)], 0)

    def pair_copy(i, target):
        return pltpu.make_async_remote_copy(
            src_ref=state_out.at[i],
            dst_ref=state_in.at[i],
            send_sem=pair_out.at[i],
            recv_sem=pair_in.at[i],
            device_id=place(target, sq),
            device_id_type=pl.DeviceIdType.MESH,
        )

    def even_copy(sender, target):
        return pltpu.make_async_remote_copy(
            src_ref=state_out.at[2],
            dst_ref=even_in.at[sender],
            send_sem=even_out_sem.at[target],
            recv_sem=even_in_sem.at[sender],
            device_id=place(2 * target, sq),
            device_id_type=pl.DeviceIdType.MESH,
        )

    def pack(i, total):
        state_out[i, :heads] = total[:heads].astype(BF16)
        state_out[i, heads], state_out[i, heads + 1] = halves(total[heads] + total[heads + 1])

    def set_states(total):
        norms = total[heads] + total[heads + 1]
        for h in range(heads):
            sin[h] = total[h]
            nin[h] = spread(jnp.where(lane == h, norms, 0.0))

    pair, pairs = me // 2, peers // 2

    def own_states():
        packed = jnp.zeros((rank, width), F32)
        for h in range(heads):
            own[h] = sum(sall[e, h] for e in ext)
            packed = jnp.where(lane == h, sum(nall[e, h] for e in ext), packed)
        own[heads] = packed
        own[heads + 1] = jnp.zeros((rank, width), F32)

        @pl.when(odd & (me < peers - 1))
        def _():
            pack(0, own[...])
            pair_copy(0, me + 1).start()

        halo_start(odd, pieces[EARLY_ODD:])

    def pair_states():
        @pl.when(even)
        def _():
            @pl.when(me > 0)
            def _():
                pair_copy(0, me + 1).wait_recv()

            pack(2, own[...] + state_in[0].astype(F32))

            def send(p, carry):
                even_copy(pair, p).start()
                return carry

            lax.fori_loop(pair + 1, pairs, send, 0)

    def even_states():
        @pl.when(even)
        def _():
            def received(p, total):
                even_copy(p, lax.rem(pair + 1, pairs)).wait_recv()
                return total + even_in[p].astype(F32)

            total = lax.fori_loop(0, pair, received, state_in[0].astype(F32))
            pack(1, own[...] + total)
            pair_copy(1, me + 1).start()

            halo_start(even, pieces[EARLY_EVEN:])
            set_states(total)

    def odd_states():
        @pl.when(odd)
        def _():
            pair_copy(1, me - 1).wait_recv()
            set_states(state_in[1].astype(F32))

    def states_sent():
        @pl.when(even)
        def _():
            def sent(p, carry):
                even_copy(pair, p).wait_send()
                return carry

            lax.fori_loop(pair + 1, pairs, sent, 0)
            pair_copy(1, me + 1).wait_send()

        @pl.when(odd & (me < peers - 1))
        def _():
            pair_copy(0, me + 1).wait_send()

    def message(g, sender, target):
        blocks = pl.ds(0, groups[g][1] + 1)
        return pltpu.make_async_remote_copy(
            src_ref=mine.at[g, blocks],
            dst_ref=slots.at[g, sender, blocks],
            send_sem=msg_out.at[g, target],
            recv_sem=msg_in.at[g, sender],
            device_id=place(target, sq),
            device_id_type=pl.DeviceIdType.MESH,
        )

    def twice(i):
        return (lane == i) | (lane == width // 2 + i)

    def message_start(g):
        first, size = groups[g]
        every = range(1, tiles + 1)
        packed = jnp.zeros((rank, width), F32)
        for i in range(size):
            mine[g, i] = sum(dsb[j, first + i] for j in every).astype(BF16)
            packed = jnp.where(twice(i), sum(dnb[j, first + i] for j in every), packed)
        top = packed.astype(BF16).astype(F32)
        mine[g, size] = jnp.where(lane < width // 2, top, packed - top).astype(BF16)

        def send(p, carry):
            message(g, me, p).start()
            return carry

        lax.fori_loop(0, me, send, 0)

    def message_sent(g):
        def sent(p, carry):
            message(g, me, p).wait_send()
            return carry

        lax.fori_loop(0, me, sent, 0)

    def message_sum(g):
        first, size = groups[g]

        def received(p, total):
            message(g, p, lax.rem(me + 1, peers)).wait_recv()
            return total + slots[g, p, : size + 1].astype(F32)

        total = lax.fori_loop(me + 1, peers, received, jnp.zeros((size + 1, rank, width), F32))
        for i in range(size):
            gaf[first + i] = total[i]
            naf[first + i] = spread(jnp.where(twice(i), total[size], 0.0))

    def spread(x):
        return jnp.broadcast_to(jnp.sum(x, 1, keepdims=True), (rank, width))

    def over_heads(first, last, step, act):
        def block(i, carry):
            act([first + i * step + u for u in range(step)])
            return carry

        lax.fori_loop(0, (last - first) // step, block, 0)

    ext = list(range(1, tiles + 1))
    with jax.named_scope("keys"):
        loads[0].wait()
        for n in range(tiles):
            kx[:, at(n + 1)] = by_head(kin[at(n)])
    halo_start(even, pieces[first_group:EARLY_EVEN])
    with jax.named_scope("values"):
        loads[1].wait()
        for n in range(tiles):
            vx[:, at(n + 1)] = by_head(vin[at(n)])
    with jax.named_scope("maps"):
        for copy in smalls:
            copy.wait()

    def key_features(hs, tile_list):
        where = at(tile_list[0], len(tile_list))
        pre = [dot_nt(wk_ref[h], kx[h, where]) - SHIFT for h in hs]
        for h, p in zip(hs, pre):
            sigk[h, :, where] = sigmoid(p)
        return [softplus(p) for p in pre]

    def kept_part(hs, e, feat):
        return [f * (lane < count_before(h, e)).astype(F32) for f, h in zip(feat, hs)]

    def key_states(hs):
        feat = key_features(hs, ext)
        for e in ext:
            one = [f[:, (e - 1) * TILE : e * TILE] for f in feat]
            if e < tiles:
                kept = kept_part(hs, e, one)
                both = [split_dot(dot_nn, jnp.concatenate([o, k], 0), vx[h, at(e)]) for o, k, h in zip(one, kept, hs)]
                for i, h in enumerate(hs):
                    skept[e, h] = both[i][rank:]
                    nkept[e, h] = spread(kept[i])
            else:
                both = [split_dot(dot_nn, o, vx[h, at(e)]) for o, h in zip(one, hs)]
            for i, h in enumerate(hs):
                sall[e, h] = both[i][:rank]
                nall[e, h] = spread(one[i])

    with jax.named_scope("states"):
        over_heads(0, heads, UNROLL, key_states)
        own_states()

    def flip_values(hs, tile_list):
        for h in hs:
            for e in tile_list:
                vt[h, :, at(e)] = vx[h, at(e)].T

    with jax.named_scope("flip_v"):
        over_heads(0, heads, UNROLL, lambda hs: flip_values(hs, ext))
    with jax.named_scope("queries"):
        loads[2].wait()
        for n in range(tiles):
            qx[:, at(n)] = by_head(qin[at(n)])

    def query_features(hs):
        pre = [dot_nt(wq_ref[h], qx[h]) - SHIFT for h in hs]
        for h, p in zip(hs, pre):
            preq[h] = p

    with jax.named_scope("qfeat"):
        over_heads(0, heads, UNROLL, query_features)
    def weights(hs, j):
        each = range(len(hs))
        scores = [dot_nt(kx[h, at(j - 1, 2)], qx[h, at(j - 1)]) for h in hs]
        old = [jnp.where(sub < count_before(h, j - 1), scores[i][:TILE], MASKED) for i, h in enumerate(hs)]
        new = [jnp.where(causal, scores[i][TILE:], MASKED) for i in each]
        top = [jnp.max(jnp.maximum(old[i], new[i]), 0, keepdims=True) * factor for i in each]
        old = [jnp.exp2(old[i] * factor - top[i]) for i in each]
        new = [jnp.exp2(new[i] * factor - top[i]) for i in each]
        for i, h in enumerate(hs):
            rows[h, 0:1, at(j - 1)] = jnp.sum(old[i] + new[i], 0, keepdims=True)
            rows[h, 1:2, at(j - 1)] = top[i]
        return [jnp.concatenate([old[i].astype(BF16), new[i].astype(BF16)], 0) for i in each]

    def weighted(hs, j, weight):
        numer = [dot_nn(vt[h, :, at(j - 1, 2)], w) for h, w in zip(hs, weight)]
        for h, x in zip(hs, numer):
            num[h, :, at(j - 1)] = x

    def sparse(hs, j):
        weighted(hs, j, weights(hs, j))

    with jax.named_scope("sparse"):
        for j in range(2, tiles + 1):
            over_heads(0, heads, UNROLL, lambda hs, j=j: sparse(hs, j))
            if j == 2:
                with jax.named_scope("pair_states"):
                    pair_states()
    with jax.named_scope("even_states"):
        even_states()
    with jax.named_scope("cot"):
        loads[3].wait()
        for n in range(tiles):
            oh[:, at(n)] = by_head(cin[at(n)])

    def flip_cotangent(hs):
        for h in hs:
            for n in range(tiles):
                ct[h, :, at(n)] = oh[h, at(n)].T

    with jax.named_scope("flip_c"):
        over_heads(0, heads, UNROLL, flip_cotangent)
    with jax.named_scope("odd_states"):
        odd_states()

    def combine(hs, j):
        each = range(len(hs))
        where = at(j - 1)
        pre = [preq[h, :, where] for h in hs]
        feat = [softplus(p) for p in pre]
        state = [sum([sall[e, h] for e in range(1, j)], sin[h]) - skept[j - 1, h] for h in hs]
        norm = [sum([nall[e, h] for e in range(1, j)], nin[h]) - nkept[j - 1, h] for h in hs]
        decay = [jnp.exp2(-rows[h, 1:2, where]) for h in hs]
        kernel = []
        for i in each:
            fq_top, fq_low = halves(feat[i])
            st_top, st_low = halves(state[i])
            kernel.append(
                dot_tn(jnp.concatenate([st_top, st_top, st_low], 0), jnp.concatenate([fq_top, fq_low, fq_top], 0))
            )
        den = [jnp.sum(norm[i] * feat[i], 0, keepdims=True) for i in each]
        inv = [1.0 / (rows[h, 0:1, where] + decay[i] * den[i]) for i, h in enumerate(hs)]
        out = [(num[h, :, where] + decay[i] * kernel[i]) * inv[i] for i, h in enumerate(hs)]
        grad = [ct[h, :, where].astype(F32) * (decay[i] * inv[i]) for i, h in enumerate(hs)]
        dot = [jnp.sum(grad[i] * out[i], 0, keepdims=True) for i in each]
        grad = [x.astype(BF16) for x in grad]
        for i, h in enumerate(hs):
            oh[h, where] = out[i].astype(BF16).T
        d_fq = [split_dot(dot_nn, state[i], grad[i]) - norm[i] * dot[i] for i in each]
        ds = [split_dot(dot_nt, feat[i], grad[i]) for i in each]
        gq = [split_dot(dot_nn, d_fq[i] * sigmoid(pre[i]), qx[h, where]) for i, h in enumerate(hs)]
        for i, h in enumerate(hs):
            dsb[j, h] = ds[i]
            dnb[j, h] = -spread(feat[i] * dot[i])
            if j == tiles:
                grads[h] = gq[i]
            else:
                grads[h] += gq[i]

    with jax.named_scope("combine"):
        for j in range(tiles, 1, -1):
            over_heads(0, heads, UNROLL, lambda hs, j=j: combine(hs, j))

    def local_keys(hs):
        parts = [[] for _ in hs]
        for e in range(tiles):
            later = None
            if 0 < e < tiles - 1:
                later = [sum(dsb[j, h] for j in range(e + 2, tiles + 1)) for h in hs]
            near = [dsb[e + 1, h] for h in hs]
            kept = [(lane < count_before(h, e)).astype(F32) for h in hs]
            for i, h in enumerate(hs):
                values = vt[h, :, at(e)]
                if e == 0:
                    part = -kept[i] * (split_dot(dot_nn, near[i], values) + dnb[1, h])
                elif later is None:
                    part = (1.0 - kept[i]) * (split_dot(dot_nn, near[i], values) + dnb[e + 1, h])
                else:
                    both = split_dot(dot_nn, jnp.concatenate([near[i], later[i]], 0), values)
                    far = both[rank:] + sum(dnb[j, h] for j in range(e + 2, tiles + 1))
                    part = (1.0 - kept[i]) * (both[:rank] + dnb[e + 1, h]) + far
                parts[i].append(part * sigk[h, :, at(e)])
        for i, h in enumerate(hs):
            grads[heads + h] = split_dot(dot_nn, jnp.concatenate(parts[i], 1), kx[h, at(0, tiles)])

    def final_keys(hs):
        own = at(1, tiles)
        d_fk = [split_dot(dot_nn, gaf[h], vt[h, :, own]) + naf[h][:, :1] for h in hs]
        gk = [split_dot(dot_nn, d_fk[i] * sigk[h, :, own], kx[h, own]) for i, h in enumerate(hs)]
        for i, h in enumerate(hs):
            grads[heads + h] += gk[i]

    owners, stride, middle = owners_of(count, groups[-1][1])
    rounds = groups + [(heads + first, size) for first, size in groups]
    key_round = len(groups)
    ahead = flat - middle + count * stride
    part = lax.rem(ahead // stride, owners)
    inside = (flat >= middle) & (flat < middle + owners * stride) & (lax.rem(ahead, stride) == 0)

    def share(r, o):
        first, size = rounds[r]
        per = size // owners
        return pl.ds(first + o * per, per)

    def arriving(r):
        kind, g = divmod(r, key_round)
        return late_slots.at[kind, g - 1] if g else early_slots.at[kind]

    def to_owner(r, o):
        target = middle + o * stride
        return pltpu.make_async_remote_copy(
            src_ref=grads.at[share(r, o)],
            dst_ref=arriving(r).at[lax.rem(flat - target + count - 1, count)],
            send_sem=red_out.at[r],
            recv_sem=red_in.at[r],
            device_id=dict(zip(axes, divmod(target, lax.axis_size(axes[1])))),
            device_id_type=pl.DeviceIdType.MESH,
        )

    def to_all(r, where):
        return pltpu.make_async_remote_copy(
            src_ref=done.at[share(r, part)],
            dst_ref=done.at[share(r, part)],
            send_sem=back_out.at[r],
            recv_sem=back_in.at[r],
            device_id=where,
            device_id_type=pl.DeviceIdType.MESH,
        )

    def reduce_start(r):
        for o in range(owners):

            @pl.when(middle + o * stride != flat)
            def _(o=o):
                to_owner(r, o).start()

    def reduce_own(r):
        @pl.when(inside)
        def _():
            slots_now = arriving(r)
            whole_copy(slots_now, red_out.at[r], red_in.at[r]).wait_recv()
            done[share(r, part)] = grads[share(r, part)] + jnp.sum(slots_now[...], 0)
            each_other(axes, lambda where: to_all(r, where).start())

    def reduce_end(r):
        first, size = rounds[r]
        per = size // owners
        every, others = pl.ds(first, size), pl.ds(first, size - per)

        @pl.when(inside)
        def _():
            if owners > 1:
                whole_copy(done.at[others], back_out.at[r], back_in.at[r]).wait_recv()
                whole_copy(grads.at[others], red_out.at[r], red_in.at[r]).wait_send()
            whole_copy(arriving(r), back_out.at[r], back_in.at[r]).wait_send()

        @pl.when(jnp.logical_not(inside))
        def _():
            whole_copy(done.at[every], back_out.at[r], back_in.at[r]).wait_recv()
            whole_copy(grads.at[every], red_out.at[r], red_in.at[r]).wait_send()

        sums_ref[every] = done[every]

    def write_out(n):
        out_ref[at(n)] = by_head(oh[:, at(n)])

    with jax.named_scope("write_out"):
        for n in range(1, tiles):
            write_out(n)

    def first_keys(hs):
        kept = kept_part(hs, 0, key_features(hs, [0]))
        weight = weights(hs, 1)
        for i, h in enumerate(hs):
            fkept[h] = kept[i]
            prob[h] = weight[i]

    def first_values(hs):
        flip_values(hs, [0])
        kept = [fkept[h] for h in hs]
        state = [split_dot(dot_nn, k, vx[h, at(0)]) for k, h in zip(kept, hs)]
        for i, h in enumerate(hs):
            skept[0, h] = state[i]
            nkept[0, h] = spread(kept[i])
        weighted(hs, 1, [prob[h] for h in hs])
        combine(hs, 1)

    for g, (first, size) in enumerate(groups):
        last = first + size
        with jax.named_scope("halo_k"):
            halo_wait(g, 0)
        with jax.named_scope("first_keys"):
            if g == 0:
                kx[:half, at(0)] = by_head(halo[0])
            over_heads(first, last, size, first_keys)
        with jax.named_scope("halo_v"):
            halo_wait(g, 1)
        with jax.named_scope("first_values"):
            if g == 0:
                vx[:half, at(0)] = by_head(halo[1])
            over_heads(first, last, size, first_values)
        with jax.named_scope("send_ds"):
            message_start(g)
            reduce_start(g)
        with jax.named_scope("local_keys"):
            over_heads(first, last, UNROLL, local_keys)
    with jax.named_scope("write_0"):
        write_out(0)
    for g, (first, size) in enumerate(groups):
        with jax.named_scope("wait_ds"):
            message_sum(g)
        with jax.named_scope("final_keys"):
            over_heads(first, first + size, size, final_keys)
        with jax.named_scope("red_start"):
            reduce_start(key_round + g)
    with jax.named_scope("red_own"):
        for r in range(len(rounds)):
            reduce_own(r)
    with jax.named_scope("red_end"):
        for r in range(len(rounds)):
            reduce_end(r)
    with jax.named_scope("sent"):
        @pl.when(me < peers - 1)
        def _():
            whole_copy(halo, halo_out.at[0], halo_in.at[0, 0]).wait_send()
            for i, ref in enumerate((kx, vx)):
                rest = ref.at[pl.ds(half, heads - half), at(tiles)]
                whole_copy(rest, halo_out.at[1 + i], halo_in.at[0, 0]).wait_send()

        states_sent()
        for g in range(len(groups)):
            message_sent(g)


def finish_kernel(rows_ref, sums_ref, out_hbm, gq_hbm, gk_hbm, sem):
    heads = gq_hbm.shape[0]
    tokens = rows_ref.shape[0] // PARTS
    copies = [
        pltpu.make_async_copy(sums_ref.at[pl.ds(0, heads)], gq_hbm, sem.at[PARTS]),
        pltpu.make_async_copy(sums_ref.at[pl.ds(heads, heads)], gk_hbm, sem.at[PARTS + 1]),
    ]
    for i in range(PARTS):
        some = pl.ds(i * tokens, tokens)
        copies.append(pltpu.make_async_copy(rows_ref.at[some], out_hbm.at[some], sem.at[i]))
    for copy in copies:
        copy.start()
    for copy in copies:
        copy.wait()


def body(queries, keys, values, keep_count, query_map, key_map, cotangent):
    q_rows, k_rows, v_rows, cot = queries[0], keys[0], values[0], cotangent[0]
    tokens, heads, width = q_rows.shape
    rank = query_map.shape[2]
    tiles = tokens // TILE
    axes = ("seq", "batch")
    peers = lax.axis_size("seq")
    count = peers * lax.axis_size("batch")
    half, quarter = groups_of(heads)[0][1], groups_of(heads)[-1][1]
    owners, _, _ = owners_of(count, quarter)
    hbm = pl.BlockSpec(memory_space=pltpu.HBM)
    vmem = pl.BlockSpec(memory_space=pltpu.VMEM)
    dma = pltpu.SemaphoreType.DMA
    small = pltpu.VMEM((heads, rank, width), F32)
    tiled = pltpu.VMEM((tiles + 1, heads, rank, width), F32)
    states = (heads + 2, rank, width)
    packed = pltpu.VMEM((heads, rank, width), BF16)
    operands = [keep_count[0], q_rows, k_rows, v_rows, cot, jnp.swapaxes(query_map, 1, 2), jnp.swapaxes(key_map, 1, 2)]
    rows, sums = pl.pallas_call(
        functools.partial(layer_kernel, "seq", axes),
        name="layer",
        in_specs=[hbm] * 7,
        out_specs=[vmem, vmem],
        out_shape=[
            jax.ShapeDtypeStruct((tokens, heads, width), BF16),
            jax.ShapeDtypeStruct((2 * heads, rank, width), F32),
        ],
        scratch_shapes=[pltpu.VMEM((tokens, heads, width), BF16)] * 4
        + [pltpu.VMEM((heads, tokens + TILE, width), BF16)] * 2
        + [
            pltpu.VMEM((heads, width, tokens + TILE), BF16),
            pltpu.VMEM((heads, tokens, width), BF16),
            pltpu.VMEM((heads, width, tokens), BF16),
            pltpu.VMEM((heads, tokens, width), BF16),
            pltpu.VMEM((2, TILE, half, width), BF16),
            pltpu.VMEM((heads, width, tokens), F32),
            pltpu.VMEM((heads, 8, tokens), F32),
            pltpu.VMEM((heads, rank, tokens), F32),
            pltpu.VMEM((heads, rank, tokens + TILE), F32),
            tiled, tiled, tiled, tiled, small, small, tiled, tiled, small, small,
            pltpu.SMEM(keep_count.shape[1:], jnp.int32),
            packed, packed,
            pltpu.VMEM((heads, 2 * TILE, TILE), BF16),
            small,
            pltpu.VMEM((2, TILE, half, width), BF16),
            pltpu.VMEM(states, F32),
            pltpu.VMEM((3,) + states, BF16),
            pltpu.VMEM((2,) + states, BF16),
            pltpu.VMEM((peers // 2,) + states, BF16),
            pltpu.VMEM((3, half + 1, rank, width), BF16),
            pltpu.VMEM((3, peers, half + 1, rank, width), BF16),
            pltpu.VMEM((2 * heads, rank, width), F32),
            pltpu.VMEM((2, count - 1, half // owners, rank, width), F32),
            pltpu.VMEM((2, 2, count - 1, quarter // owners, rank, width), F32),
            pltpu.VMEM((2 * heads, rank, width), F32),
            dma((4,)), dma((2,)), dma((3,)), dma((3,)), dma((3, 2)), dma((2,)), dma((2,)),
            dma((peers // 2,)), dma((peers // 2,)), dma((3, peers)), dma((3, peers)),
            dma((6,)), dma((6,)), dma((6,)), dma((6,)),
        ],
        compiler_params=pltpu.CompilerParams(
            collective_id=0, has_side_effects=True, vmem_limit_bytes=VMEM_LIMIT
        ),
    )(*[pltpu.with_memory_space_constraint(x, pltpu.HBM) for x in operands])
    out, gq, gk = pl.pallas_call(
        finish_kernel,
        name="finish",
        in_specs=[vmem, vmem],
        out_specs=[hbm, hbm, hbm],
        out_shape=[
            jax.ShapeDtypeStruct((tokens, heads, width), BF16),
            jax.ShapeDtypeStruct((heads, rank, width), F32),
            jax.ShapeDtypeStruct((heads, rank, width), F32),
        ],
        scratch_shapes=[dma((PARTS + 2,))],
        compiler_params=pltpu.CompilerParams(vmem_limit_bytes=VMEM_LIMIT),
    )(rows, sums)
    return out[None], jnp.swapaxes(gq, 1, 2), jnp.swapaxes(gk, 1, 2)


def solution(mesh):
    placed = (
        P("batch", "seq", None, None),
        P("batch", "seq", None, None),
        P("batch", "seq", None, None),
        P("batch", None, None),
        P(),
        P(),
        P("batch", "seq", None, None),
    )
    return jax.shard_map(
        body,
        mesh=mesh,
        in_specs=placed,
        out_specs=(P("batch", "seq", None, None), P(), P()),
        check_vma=False,
    )
```

```python
import functools
import math

import jax
import jax.numpy as jnp
from jax import lax
from jax.experimental import pallas as pl
from jax.experimental.pallas import tpu as pltpu
from jax.sharding import PartitionSpec as P

TILE = 128
SHIFT = 1.5
LOG2E = 1.0 / math.log(2.0)
MASKED = -1e30
F32 = jnp.float32
BF16 = jnp.bfloat16
UNROLL = 8
CUTS = 4
EARLY_EVEN = 9
EARLY_ODD = 3
PARTS = 4
VMEM_LIMIT = 50 * 1024 * 1024


def dot_nt(a, b):
    return lax.dot_general(a, b, (((1,), (1,)), ((), ())), preferred_element_type=F32)


def dot_nn(a, b):
    return lax.dot_general(a, b, (((1,), (0,)), ((), ())), preferred_element_type=F32)


def dot_tn(a, b):
    return lax.dot_general(a, b, (((0,), (0,)), ((), ())), preferred_element_type=F32)


def by_head(x):
    return jnp.swapaxes(x, 0, 1)


def softplus(x):
    return jnp.maximum(x, 0.0) + jnp.log1p(jnp.exp(-jnp.abs(x)))


def sigmoid(x):
    return 1.0 / (1.0 + jnp.exp(-x))


def halves(x):
    top = x.astype(BF16)
    return top, (x - top.astype(F32)).astype(BF16)


def split_dot(dot, x, y):
    rows = x.shape[0]
    both = dot(jnp.concatenate(halves(x), 0), y)
    return both[:rows] + both[rows:]


def flat_id(axes):
    index, count = 0, 1
    for axis in axes:
        index = index * lax.axis_size(axis) + lax.axis_index(axis)
        count *= lax.axis_size(axis)
    return index, count


def place(flat, axes):
    where = {}
    for axis in reversed(axes):
        size = lax.axis_size(axis)
        where[axis] = lax.rem(flat, size)
        flat = flat // size
    return where


def each_other(axes, act):
    outer, inner = axes
    me, mine = lax.axis_index(outer), lax.axis_index(inner)
    peers, others = lax.axis_size(outer), lax.axis_size(inner)

    def far(i, carry):
        s = me + i
        s = jnp.where(s >= peers, s - peers, s)
        for b in range(others):
            act({outer: s, inner: b})
        return carry

    lax.fori_loop(1, peers, far, 0)
    for b in range(others):

        @pl.when(mine != b)
        def _(b=b):
            act({outer: me, inner: b})


def greet(axes):
    barrier = pltpu.get_barrier_semaphore()
    each_other(
        axes,
        lambda where: pl.semaphore_signal(barrier, inc=1, device_id=where, device_id_type=pl.DeviceIdType.MESH),
    )
    return barrier


def at(tile, count=1):
    return pl.ds(tile * TILE, count * TILE)


def groups_of(heads):
    half, quarter = heads // 2, heads // 4
    return [(0, half), (half, quarter), (half + quarter, quarter)]


def owners_of(count, chunks):
    owners = min(count, chunks)
    stride = 2 if count >= 2 * owners else 1
    return owners, stride, (count - owners * stride) // 2 + stride - 1


def layer_kernel(
    seq, axes, counts_hbm, q_hbm, k_hbm, v_hbm, c_hbm, wq_hbm, wk_hbm, out_ref, sums_ref,
    qin, kin, vin, cin, kx, vx, vt, qx, ct, oh, halo, num, rows, preq, sigk, sall, nall, skept, nkept,
    sin, nin, dsb, dnb, gaf, naf, counts_ref, wq_ref, wk_ref, prob, fkept, sent_halo,
    own, state_out, state_in, even_in, mine, slots, grads, early_slots, late_slots, done,
    in_sem, edge_sem, small_sem, halo_out, halo_in, pair_out, pair_in, even_out_sem, even_in_sem,
    msg_out, msg_in, red_out, red_in, back_out, back_in,
):
    tokens, heads, width = q_hbm.shape
    rank = wq_hbm.shape[1]
    tiles = tokens // TILE
    groups = groups_of(heads)
    half = groups[0][1]
    factor = LOG2E / math.sqrt(width)
    me = lax.axis_index(seq)
    peers = lax.axis_size(seq)
    flat, count = flat_id(axes)
    sq = (seq,)
    barrier = greet(axes)
    base = me * tiles
    lane = lax.broadcasted_iota(jnp.int32, (1, TILE), 1)
    sub = lax.broadcasted_iota(jnp.int32, (TILE, TILE), 0)
    causal = sub <= lax.broadcasted_iota(jnp.int32, (TILE, TILE), 1)

    early = [
        pltpu.make_async_copy(
            hbm.at[pl.ds(tokens - TILE, TILE), pl.ds(0, half)], sent_halo.at[i], edge_sem.at[i]
        )
        for i, hbm in enumerate((k_hbm, v_hbm))
    ]
    for copy in early:
        copy.start()
    pairs_in = [(k_hbm, kin), (v_hbm, vin), (q_hbm, qin), (c_hbm, cin)]
    loads = [pltpu.make_async_copy(hbm, vmem, in_sem.at[i]) for i, (hbm, vmem) in enumerate(pairs_in)]
    for copy in loads:
        copy.start()

    smalls = [
        pltpu.make_async_copy(counts_hbm, counts_ref, small_sem.at[0]),
        pltpu.make_async_copy(wk_hbm, wk_ref, small_sem.at[1]),
        pltpu.make_async_copy(wq_hbm, wq_ref, small_sem.at[2]),
    ]
    for copy in smalls:
        copy.start()

    @pl.when(me == 0)
    def _():
        halo[...] = jnp.zeros_like(halo)
        blank = jnp.zeros((heads - half, TILE, width), BF16)
        kx[half:, at(0)] = blank
        vx[half:, at(0)] = blank
        state_in[0] = jnp.zeros_like(state_in[0])

    even = lax.rem(me, 2) == 0
    cut = TILE // CUTS
    pieces = [(0, i, r) for i in range(2) for r in range(CUTS)]
    for g, (first, size) in enumerate(groups[1:], 1):
        pieces += [(g, i, h) for i in range(2) for h in range(first, first + size, 2)]

    def halo_copy(g, i, r):
        if g:
            both = (kx, vx)[i].at[pl.ds(r, 2)]
            src, dst = both.at[:, at(tiles)], both.at[:, at(0)]
        else:
            src, dst = sent_halo.at[i, pl.ds(r * cut, cut)], halo.at[i, pl.ds(r * cut, cut)]
        return pltpu.make_async_remote_copy(
            src_ref=src,
            dst_ref=dst,
            send_sem=halo_out.at[1 + i if g else 0],
            recv_sem=halo_in.at[g, i],
            device_id=place(lax.rem(me + 1, peers), sq),
            device_id_type=pl.DeviceIdType.MESH,
        )

    def whole_copy(ref, send_sem, recv_sem):
        return pltpu.make_async_remote_copy(
            src_ref=ref,
            dst_ref=ref,
            send_sem=send_sem,
            recv_sem=recv_sem,
            device_id=place(lax.rem(me + 1, peers), sq),
            device_id_type=pl.DeviceIdType.MESH,
        )

    def halo_wait(g, i):
        @pl.when(me > 0)
        def _():
            landed = (kx, vx)[i].at[pl.ds(*groups[g]), at(0)] if g else halo.at[i]
            whole_copy(landed, halo_out.at[0], halo_in.at[g, i]).wait_recv()

    for copy in early:
        copy.wait()
    with jax.named_scope("barrier"):
        pl.semaphore_wait(barrier, count - 1)

    def halo_start(mine, some):
        @pl.when(mine & (me < peers - 1))
        def _():
            for piece in some:
                halo_copy(*piece).start()

    odd = jnp.logical_not(even)
    first_group = 2 * CUTS
    halo_start(even, pieces[:first_group])
    halo_start(odd, pieces[:EARLY_ODD])

    def count_before(h, e):
        if e:
            return counts_ref[h, base + e - 1]
        return jnp.where(me > 0, counts_ref[h, jnp.maximum(base - 1, 0)], 0)

    def pair_copy(i, target):
        return pltpu.make_async_remote_copy(
            src_ref=state_out.at[i],
            dst_ref=state_in.at[i],
            send_sem=pair_out.at[i],
            recv_sem=pair_in.at[i],
            device_id=place(target, sq),
            device_id_type=pl.DeviceIdType.MESH,
        )

    def even_copy(sender, target):
        return pltpu.make_async_remote_copy(
            src_ref=state_out.at[2],
            dst_ref=even_in.at[sender],
            send_sem=even_out_sem.at[target],
            recv_sem=even_in_sem.at[sender],
            device_id=place(2 * target, sq),
            device_id_type=pl.DeviceIdType.MESH,
        )

    def pack(i, total):
        state_out[i, :heads] = total[:heads].astype(BF16)
        state_out[i, heads], state_out[i, heads + 1] = halves(total[heads] + total[heads + 1])

    def set_states(total):
        norms = total[heads] + total[heads + 1]
        for h in range(heads):
            sin[h] = total[h]
            nin[h] = spread(jnp.where(lane == h, norms, 0.0))

    pair, pairs = me // 2, peers // 2

    def own_states():
        packed = jnp.zeros((rank, width), F32)
        for h in range(heads):
            own[h] = sum(sall[e, h] for e in ext)
            packed = jnp.where(lane == h, sum(nall[e, h] for e in ext), packed)
        own[heads] = packed
        own[heads + 1] = jnp.zeros((rank, width), F32)

        @pl.when(odd & (me < peers - 1))
        def _():
            pack(0, own[...])
            pair_copy(0, me + 1).start()

        halo_start(odd, pieces[EARLY_ODD:])

    def pair_states():
        @pl.when(even)
        def _():
            @pl.when(me > 0)
            def _():
                pair_copy(0, me + 1).wait_recv()

            pack(2, own[...] + state_in[0].astype(F32))

            def send(p, carry):
                even_copy(pair, p).start()
                return carry

            lax.fori_loop(pair + 1, pairs, send, 0)

    def even_states():
        @pl.when(even)
        def _():
            def received(p, total):
                even_copy(p, lax.rem(pair + 1, pairs)).wait_recv()
                return total + even_in[p].astype(F32)

            total = lax.fori_loop(0, pair, received, state_in[0].astype(F32))
            pack(1, own[...] + total)
            pair_copy(1, me + 1).start()

            halo_start(even, pieces[EARLY_EVEN:])
            set_states(total)

    def odd_states():
        @pl.when(odd)
        def _():
            pair_copy(1, me - 1).wait_recv()
            set_states(state_in[1].astype(F32))

    def states_sent():
        @pl.when(even)
        def _():
            def sent(p, carry):
                even_copy(pair, p).wait_send()
                return carry

            lax.fori_loop(pair + 1, pairs, sent, 0)
            pair_copy(1, me + 1).wait_send()

        @pl.when(odd & (me < peers - 1))
        def _():
            pair_copy(0, me + 1).wait_send()

    def message(g, sender, target):
        blocks = pl.ds(0, groups[g][1] + 1)
        return pltpu.make_async_remote_copy(
            src_ref=mine.at[g, blocks],
            dst_ref=slots.at[g, sender, blocks],
            send_sem=msg_out.at[g, target],
            recv_sem=msg_in.at[g, sender],
            device_id=place(target, sq),
            device_id_type=pl.DeviceIdType.MESH,
        )

    def twice(i):
        return (lane == i) | (lane == width // 2 + i)

    def message_start(g):
        first, size = groups[g]
        every = range(1, tiles + 1)
        packed = jnp.zeros((rank, width), F32)
        for i in range(size):
            mine[g, i] = sum(dsb[j, first + i] for j in every).astype(BF16)
            packed = jnp.where(twice(i), sum(dnb[j, first + i] for j in every), packed)
        top = packed.astype(BF16).astype(F32)
        mine[g, size] = jnp.where(lane < width // 2, top, packed - top).astype(BF16)

        def send(p, carry):
            message(g, me, p).start()
            return carry

        lax.fori_loop(0, me, send, 0)

    def message_sent(g):
        def sent(p, carry):
            message(g, me, p).wait_send()
            return carry

        lax.fori_loop(0, me, sent, 0)

    def message_sum(g):
        first, size = groups[g]

        def received(p, total):
            message(g, p, lax.rem(me + 1, peers)).wait_recv()
            return total + slots[g, p, : size + 1].astype(F32)

        total = lax.fori_loop(me + 1, peers, received, jnp.zeros((size + 1, rank, width), F32))
        for i in range(size):
            gaf[first + i] = total[i]
            naf[first + i] = spread(jnp.where(twice(i), total[size], 0.0))

    def spread(x):
        return jnp.broadcast_to(jnp.sum(x, 1, keepdims=True), (rank, width))

    def over_heads(first, last, step, act):
        step = min(step, last - first)

        def block(i, carry):
            act([first + i * step + u for u in range(step)])
            return carry

        lax.fori_loop(0, (last - first) // step, block, 0)

    ext = list(range(1, tiles + 1))
    with jax.named_scope("keys"):
        loads[0].wait()
        for n in range(tiles):
            kx[:, at(n + 1)] = by_head(kin[at(n)])
    halo_start(even, pieces[first_group:EARLY_EVEN])
    with jax.named_scope("values"):
        loads[1].wait()
        for n in range(tiles):
            vx[:, at(n + 1)] = by_head(vin[at(n)])
    with jax.named_scope("maps"):
        for copy in smalls:
            copy.wait()

    def key_features(hs, tile_list):
        where = at(tile_list[0], len(tile_list))
        pre = [dot_nt(wk_ref[h], kx[h, where]) - SHIFT for h in hs]
        for h, p in zip(hs, pre):
            sigk[h, :, where] = sigmoid(p)
        return [softplus(p) for p in pre]

    def kept_part(hs, e, feat):
        return [f * (lane < count_before(h, e)).astype(F32) for f, h in zip(feat, hs)]

    def key_states(hs):
        feat = key_features(hs, ext)
        for e in ext:
            one = [f[:, (e - 1) * TILE : e * TILE] for f in feat]
            if e < tiles:
                kept = kept_part(hs, e, one)
                both = [split_dot(dot_nn, jnp.concatenate([o, k], 0), vx[h, at(e)]) for o, k, h in zip(one, kept, hs)]
                for i, h in enumerate(hs):
                    skept[e, h] = both[i][rank:]
                    nkept[e, h] = spread(kept[i])
            else:
                both = [split_dot(dot_nn, o, vx[h, at(e)]) for o, h in zip(one, hs)]
            for i, h in enumerate(hs):
                sall[e, h] = both[i][:rank]
                nall[e, h] = spread(one[i])

    with jax.named_scope("states"):
        over_heads(0, heads, UNROLL, key_states)
        own_states()

    def flip_values(hs, tile_list):
        for h in hs:
            for e in tile_list:
                vt[h, :, at(e)] = vx[h, at(e)].T

    with jax.named_scope("flip_v"):
        over_heads(0, heads, UNROLL, lambda hs: flip_values(hs, ext))
    with jax.named_scope("queries"):
        loads[2].wait()
        for n in range(tiles):
            qx[:, at(n)] = by_head(qin[at(n)])

    def query_features(hs):
        pre = [dot_nt(wq_ref[h], qx[h]) - SHIFT for h in hs]
        for h, p in zip(hs, pre):
            preq[h] = p

    with jax.named_scope("qfeat"):
        over_heads(0, heads, UNROLL, query_features)
    def weights(hs, j):
        each = range(len(hs))
        scores = [dot_nt(kx[h, at(j - 1, 2)], qx[h, at(j - 1)]) for h in hs]
        old = [jnp.where(sub < count_before(h, j - 1), scores[i][:TILE], MASKED) for i, h in enumerate(hs)]
        new = [jnp.where(causal, scores[i][TILE:], MASKED) for i in each]
        top = [jnp.max(jnp.maximum(old[i], new[i]), 0, keepdims=True) * factor for i in each]
        old = [jnp.exp2(old[i] * factor - top[i]) for i in each]
        new = [jnp.exp2(new[i] * factor - top[i]) for i in each]
        for i, h in enumerate(hs):
            rows[h, 0:1, at(j - 1)] = jnp.sum(old[i] + new[i], 0, keepdims=True)
            rows[h, 1:2, at(j - 1)] = top[i]
        return [jnp.concatenate([old[i].astype(BF16), new[i].astype(BF16)], 0) for i in each]

    def weighted(hs, j, weight):
        numer = [dot_nn(vt[h, :, at(j - 1, 2)], w) for h, w in zip(hs, weight)]
        for h, x in zip(hs, numer):
            num[h, :, at(j - 1)] = x

    def sparse(hs, j):
        weighted(hs, j, weights(hs, j))

    with jax.named_scope("sparse"):
        for j in range(2, tiles + 1):
            over_heads(0, heads, UNROLL, lambda hs, j=j: sparse(hs, j))
            if j == 2:
                with jax.named_scope("pair_states"):
                    pair_states()
    with jax.named_scope("even_states"):
        even_states()
    with jax.named_scope("cot"):
        loads[3].wait()
        for n in range(tiles):
            oh[:, at(n)] = by_head(cin[at(n)])

    def flip_cotangent(hs):
        for h in hs:
            for n in range(tiles):
                ct[h, :, at(n)] = oh[h, at(n)].T

    with jax.named_scope("flip_c"):
        over_heads(0, heads, UNROLL, flip_cotangent)
    with jax.named_scope("odd_states"):
        odd_states()

    def combine(hs, j):
        each = range(len(hs))
        where = at(j - 1)
        pre = [preq[h, :, where] for h in hs]
        feat = [softplus(p) for p in pre]
        state = [sum([sall[e, h] for e in range(1, j)], sin[h]) - skept[j - 1, h] for h in hs]
        norm = [sum([nall[e, h] for e in range(1, j)], nin[h]) - nkept[j - 1, h] for h in hs]
        decay = [jnp.exp2(-rows[h, 1:2, where]) for h in hs]
        kernel = []
        for i in each:
            fq_top, fq_low = halves(feat[i])
            st_top, st_low = halves(state[i])
            kernel.append(
                dot_tn(jnp.concatenate([st_top, st_top, st_low], 0), jnp.concatenate([fq_top, fq_low, fq_top], 0))
            )
        den = [jnp.sum(norm[i] * feat[i], 0, keepdims=True) for i in each]
        inv = [1.0 / (rows[h, 0:1, where] + decay[i] * den[i]) for i, h in enumerate(hs)]
        out = [(num[h, :, where] + decay[i] * kernel[i]) * inv[i] for i, h in enumerate(hs)]
        grad = [ct[h, :, where].astype(F32) * (decay[i] * inv[i]) for i, h in enumerate(hs)]
        dot = [jnp.sum(grad[i] * out[i], 0, keepdims=True) for i in each]
        grad = [x.astype(BF16) for x in grad]
        for i, h in enumerate(hs):
            oh[h, where] = out[i].astype(BF16).T
        d_fq = [split_dot(dot_nn, state[i], grad[i]) - norm[i] * dot[i] for i in each]
        ds = [split_dot(dot_nt, feat[i], grad[i]) for i in each]
        gq = [split_dot(dot_nn, d_fq[i] * sigmoid(pre[i]), qx[h, where]) for i, h in enumerate(hs)]
        for i, h in enumerate(hs):
            dsb[j, h] = ds[i]
            dnb[j, h] = -spread(feat[i] * dot[i])
            if j == tiles:
                grads[h] = gq[i]
            else:
                grads[h] += gq[i]

    with jax.named_scope("combine"):
        for j in range(tiles, 1, -1):
            over_heads(0, heads, UNROLL, lambda hs, j=j: combine(hs, j))

    def local_keys(hs):
        parts = [[] for _ in hs]
        for e in range(tiles):
            later = None
            if 0 < e < tiles - 1:
                later = [sum(dsb[j, h] for j in range(e + 2, tiles + 1)) for h in hs]
            near = [dsb[e + 1, h] for h in hs]
            kept = [(lane < count_before(h, e)).astype(F32) for h in hs]
            for i, h in enumerate(hs):
                values = vt[h, :, at(e)]
                if e == 0:
                    part = -kept[i] * (split_dot(dot_nn, near[i], values) + dnb[1, h])
                elif later is None:
                    part = (1.0 - kept[i]) * (split_dot(dot_nn, near[i], values) + dnb[e + 1, h])
                else:
                    both = split_dot(dot_nn, jnp.concatenate([near[i], later[i]], 0), values)
                    far = both[rank:] + sum(dnb[j, h] for j in range(e + 2, tiles + 1))
                    part = (1.0 - kept[i]) * (both[:rank] + dnb[e + 1, h]) + far
                parts[i].append(part * sigk[h, :, at(e)])
        for i, h in enumerate(hs):
            grads[heads + h] = split_dot(dot_nn, jnp.concatenate(parts[i], 1), kx[h, at(0, tiles)])

    def final_keys(hs):
        own = at(1, tiles)
        d_fk = [split_dot(dot_nn, gaf[h], vt[h, :, own]) + naf[h][:, :1] for h in hs]
        gk = [split_dot(dot_nn, d_fk[i] * sigk[h, :, own], kx[h, own]) for i, h in enumerate(hs)]
        for i, h in enumerate(hs):
            grads[heads + h] += gk[i]

    owners, stride, middle = owners_of(count, groups[-1][1])
    rounds = groups + [(heads + first, size) for first, size in groups]
    key_round = len(groups)
    ahead = flat - middle + count * stride
    part = lax.rem(ahead // stride, owners)
    inside = (flat >= middle) & (flat < middle + owners * stride) & (lax.rem(ahead, stride) == 0)

    def share(r, o):
        first, size = rounds[r]
        per = size // owners
        return pl.ds(first + o * per, per)

    def arriving(r):
        kind, g = divmod(r, key_round)
        return late_slots.at[kind, g - 1] if g else early_slots.at[kind]

    def to_owner(r, o):
        target = middle + o * stride
        return pltpu.make_async_remote_copy(
            src_ref=grads.at[share(r, o)],
            dst_ref=arriving(r).at[lax.rem(flat - target + count - 1, count)],
            send_sem=red_out.at[r],
            recv_sem=red_in.at[r],
            device_id=dict(zip(axes, divmod(target, lax.axis_size(axes[1])))),
            device_id_type=pl.DeviceIdType.MESH,
        )

    def to_all(r, where):
        return pltpu.make_async_remote_copy(
            src_ref=done.at[share(r, part)],
            dst_ref=done.at[share(r, part)],
            send_sem=back_out.at[r],
            recv_sem=back_in.at[r],
            device_id=where,
            device_id_type=pl.DeviceIdType.MESH,
        )

    def reduce_start(r):
        for o in range(owners):

            @pl.when(middle + o * stride != flat)
            def _(o=o):
                to_owner(r, o).start()

    def reduce_own(r):
        @pl.when(inside)
        def _():
            slots_now = arriving(r)
            whole_copy(slots_now, red_out.at[r], red_in.at[r]).wait_recv()
            done[share(r, part)] = grads[share(r, part)] + jnp.sum(slots_now[...], 0)
            each_other(axes, lambda where: to_all(r, where).start())

    def reduce_end(r):
        first, size = rounds[r]
        per = size // owners
        every, others = pl.ds(first, size), pl.ds(first, size - per)

        @pl.when(inside)
        def _():
            if owners > 1:
                whole_copy(done.at[others], back_out.at[r], back_in.at[r]).wait_recv()
                whole_copy(grads.at[others], red_out.at[r], red_in.at[r]).wait_send()
            whole_copy(arriving(r), back_out.at[r], back_in.at[r]).wait_send()

        @pl.when(jnp.logical_not(inside))
        def _():
            whole_copy(done.at[every], back_out.at[r], back_in.at[r]).wait_recv()
            whole_copy(grads.at[every], red_out.at[r], red_in.at[r]).wait_send()

        sums_ref[every] = done[every]

    def write_out(n):
        out_ref[at(n)] = by_head(oh[:, at(n)])

    with jax.named_scope("write_out"):
        for n in range(1, tiles):
            write_out(n)

    def first_keys(hs):
        kept = kept_part(hs, 0, key_features(hs, [0]))
        weight = weights(hs, 1)
        for i, h in enumerate(hs):
            fkept[h] = kept[i]
            prob[h] = weight[i]

    def first_values(hs):
        flip_values(hs, [0])
        kept = [fkept[h] for h in hs]
        state = [split_dot(dot_nn, k, vx[h, at(0)]) for k, h in zip(kept, hs)]
        for i, h in enumerate(hs):
            skept[0, h] = state[i]
            nkept[0, h] = spread(kept[i])
        weighted(hs, 1, [prob[h] for h in hs])
        combine(hs, 1)

    for g, (first, size) in enumerate(groups):
        last = first + size
        with jax.named_scope("halo_k"):
            halo_wait(g, 0)
        with jax.named_scope("first_keys"):
            if g == 0:
                kx[:half, at(0)] = by_head(halo[0])
            over_heads(first, last, size, first_keys)
        with jax.named_scope("halo_v"):
            halo_wait(g, 1)
        with jax.named_scope("first_values"):
            if g == 0:
                vx[:half, at(0)] = by_head(halo[1])
            over_heads(first, last, size, first_values)
        with jax.named_scope("send_ds"):
            message_start(g)
            reduce_start(g)
        with jax.named_scope("local_keys"):
            over_heads(first, last, UNROLL, local_keys)
    with jax.named_scope("write_0"):
        write_out(0)
    for g, (first, size) in enumerate(groups):
        with jax.named_scope("wait_ds"):
            message_sum(g)
        with jax.named_scope("final_keys"):
            over_heads(first, first + size, size, final_keys)
        with jax.named_scope("red_start"):
            reduce_start(key_round + g)
    with jax.named_scope("red_own"):
        for r in range(len(rounds)):
            reduce_own(r)
    with jax.named_scope("red_end"):
        for r in range(len(rounds)):
            reduce_end(r)
    with jax.named_scope("sent"):
        @pl.when(me < peers - 1)
        def _():
            whole_copy(halo, halo_out.at[0], halo_in.at[0, 0]).wait_send()
            for i, ref in enumerate((kx, vx)):
                rest = ref.at[pl.ds(half, heads - half), at(tiles)]
                whole_copy(rest, halo_out.at[1 + i], halo_in.at[0, 0]).wait_send()

        states_sent()
        for g in range(len(groups)):
            message_sent(g)


def finish_kernel(rows_ref, sums_ref, out_hbm, gq_hbm, gk_hbm, sem):
    heads = gq_hbm.shape[0]
    tokens = rows_ref.shape[0] // PARTS
    copies = [
        pltpu.make_async_copy(sums_ref.at[pl.ds(0, heads)], gq_hbm, sem.at[PARTS]),
        pltpu.make_async_copy(sums_ref.at[pl.ds(heads, heads)], gk_hbm, sem.at[PARTS + 1]),
    ]
    for i in range(PARTS):
        some = pl.ds(i * tokens, tokens)
        copies.append(pltpu.make_async_copy(rows_ref.at[some], out_hbm.at[some], sem.at[i]))
    for copy in copies:
        copy.start()
    for copy in copies:
        copy.wait()


def body(queries, keys, values, keep_count, query_map, key_map, cotangent):
    q_rows, k_rows, v_rows, cot = queries[0], keys[0], values[0], cotangent[0]
    tokens, heads, width = q_rows.shape
    rank = query_map.shape[2]
    tiles = tokens // TILE
    axes = ("seq", "batch")
    peers = lax.axis_size("seq")
    count = peers * lax.axis_size("batch")
    half, quarter = groups_of(heads)[0][1], groups_of(heads)[-1][1]
    owners, _, _ = owners_of(count, quarter)
    hbm = pl.BlockSpec(memory_space=pltpu.HBM)
    vmem = pl.BlockSpec(memory_space=pltpu.VMEM)
    dma = pltpu.SemaphoreType.DMA
    small = pltpu.VMEM((heads, rank, width), F32)
    tiled = pltpu.VMEM((tiles + 1, heads, rank, width), F32)
    states = (heads + 2, rank, width)
    packed = pltpu.VMEM((heads, rank, width), BF16)
    operands = [keep_count[0], q_rows, k_rows, v_rows, cot, jnp.swapaxes(query_map, 1, 2), jnp.swapaxes(key_map, 1, 2)]
    rows, sums = pl.pallas_call(
        functools.partial(layer_kernel, "seq", axes),
        name="layer",
        in_specs=[hbm] * 7,
        out_specs=[vmem, vmem],
        out_shape=[
            jax.ShapeDtypeStruct((tokens, heads, width), BF16),
            jax.ShapeDtypeStruct((2 * heads, rank, width), F32),
        ],
        scratch_shapes=[pltpu.VMEM((tokens, heads, width), BF16)] * 4
        + [pltpu.VMEM((heads, tokens + TILE, width), BF16)] * 2
        + [
            pltpu.VMEM((heads, width, tokens + TILE), BF16),
            pltpu.VMEM((heads, tokens, width), BF16),
            pltpu.VMEM((heads, width, tokens), BF16),
            pltpu.VMEM((heads, tokens, width), BF16),
            pltpu.VMEM((2, TILE, half, width), BF16),
            pltpu.VMEM((heads, width, tokens), F32),
            pltpu.VMEM((heads, 8, tokens), F32),
            pltpu.VMEM((heads, rank, tokens), F32),
            pltpu.VMEM((heads, rank, tokens + TILE), F32),
            tiled, tiled, tiled, tiled, small, small, tiled, tiled, small, small,
            pltpu.SMEM(keep_count.shape[1:], jnp.int32),
            packed, packed,
            pltpu.VMEM((heads, 2 * TILE, TILE), BF16),
            small,
            pltpu.VMEM((2, TILE, half, width), BF16),
            pltpu.VMEM(states, F32),
            pltpu.VMEM((3,) + states, BF16),
            pltpu.VMEM((2,) + states, BF16),
            pltpu.VMEM((peers // 2,) + states, BF16),
            pltpu.VMEM((3, half + 1, rank, width), BF16),
            pltpu.VMEM((3, peers, half + 1, rank, width), BF16),
            pltpu.VMEM((2 * heads, rank, width), F32),
            pltpu.VMEM((2, count - 1, half // owners, rank, width), F32),
            pltpu.VMEM((2, 2, count - 1, quarter // owners, rank, width), F32),
            pltpu.VMEM((2 * heads, rank, width), F32),
            dma((4,)), dma((2,)), dma((3,)), dma((3,)), dma((3, 2)), dma((2,)), dma((2,)),
            dma((peers // 2,)), dma((peers // 2,)), dma((3, peers)), dma((3, peers)),
            dma((6,)), dma((6,)), dma((6,)), dma((6,)),
        ],
        compiler_params=pltpu.CompilerParams(
            collective_id=0, has_side_effects=True, vmem_limit_bytes=VMEM_LIMIT
        ),
    )(*[pltpu.with_memory_space_constraint(x, pltpu.HBM) for x in operands])
    out, gq, gk = pl.pallas_call(
        finish_kernel,
        name="finish",
        in_specs=[vmem, vmem],
        out_specs=[hbm, hbm, hbm],
        out_shape=[
            jax.ShapeDtypeStruct((tokens, heads, width), BF16),
            jax.ShapeDtypeStruct((heads, rank, width), F32),
            jax.ShapeDtypeStruct((heads, rank, width), F32),
        ],
        scratch_shapes=[dma((PARTS + 2,))],
        compiler_params=pltpu.CompilerParams(vmem_limit_bytes=VMEM_LIMIT),
    )(rows, sums)
    return out[None], jnp.swapaxes(gq, 1, 2), jnp.swapaxes(gk, 1, 2)


def solution(mesh):
    placed = (
        P("batch", "seq", None, None),
        P("batch", "seq", None, None),
        P("batch", "seq", None, None),
        P("batch", None, None),
        P(),
        P(),
        P("batch", "seq", None, None),
    )
    return jax.shard_map(
        body,
        mesh=mesh,
        in_specs=placed,
        out_specs=(P("batch", "seq", None, None), P(), P()),
        check_vma=False,
    )
```
